8 devices in a mesh: dp: 1 (over z), sp: 8 (over y, x, core).
Axes of the slice: x: 2, y: 2, z: 1, core: 2. Of those that a mesh axis runs over, the one named last changes fastest.
Arguments:
- hidden: bfloat16 [32, 5120], P('dp')
- ckv_cache: bfloat16 [32, 16384, 512], P('dp', 'sp')
- kpe_cache: bfloat16 [32, 16384, 64], P('dp', 'sp')
- cache_len: int32 [32], P('dp')
- w_dq: bfloat16 [5120, 1536], replicated
- q_gain: bfloat16 [1536], replicated
- w_uq: bfloat16 [1536, 24576], replicated
- w_dkv: bfloat16 [5120, 576], replicated
- kv_gain: bfloat16 [512], replicated
- w_uk: bfloat16 [128, 128, 512], replicated
- w_uv: bfloat16 [128, 128, 512], replicated
- w_out: bfloat16 [16384, 5120], replicated
Outputs:
- output 1: bfloat16 [32, 5120], P('dp')
- output 2: bfloat16 [32, 16384, 512], P('dp', 'sp')
- output 3: bfloat16 [32, 16384, 64], P('dp', 'sp')
- output 4: bfloat16 [32, 576], P('dp')
All inputs are finite; a program needn't handle non-finite values.
Results may differ from the reference program's by a relative error of at most 0.0112942.
Values sent between devices are 32-bit elements.
A program may use at most 1.75 GiB of HBM per device.

```python
import jax
import jax.numpy as jnp
from jax import lax

D_MODEL = 5120
N_HEADS = 128
Q_LORA = 1536
KV_LORA = 512
ROPE_DIM = 64
NOPE_DIM = 128
V_DIM = 128
N_SEQS = 32
SHARD_LEN = 2048
SEQ_LEN = 16384
ROPE_THETA = 10000
N_ANCHORS = 17
EPS = 1e-6
QK_DIM = NOPE_DIM + ROPE_DIM


def rms_norm(vector, norm_gain):
    mean_sq = jnp.mean(vector * vector, axis=-1, keepdims=True)
    return vector * lax.rsqrt(mean_sq + EPS) * norm_gain.astype(jnp.float32)


def rope_tables(cache_len):
    inv_freq = jnp.power(float(ROPE_THETA), -2.0 * jnp.arange(ROPE_DIM // 2, dtype=jnp.float32) / ROPE_DIM)
    rope_angle = cache_len.astype(jnp.float32)[:, None] * inv_freq[None, :]
    return jnp.cos(rope_angle), jnp.sin(rope_angle)


def rotate(vector, cos_t, sin_t):
    half_dim = vector.shape[-1] // 2
    first_half = vector[..., :half_dim]
    second_half = vector[..., half_dim:]
    return jnp.concatenate([first_half * cos_t - second_half * sin_t, second_half * cos_t + first_half * sin_t], axis=-1)


def setup_inputs(seed: int = 0, part: int = 0) -> dict:
    part_key = jax.random.fold_in(jax.random.key(seed), part)
    hid_key, cache_key, len_key = jax.random.split(part_key, 3)
    shared = jax.random.split(jax.random.key(seed + 1), 8)
    pos_frac = jnp.arange(SEQ_LEN, dtype=jnp.float32) * ((N_ANCHORS - 1) / (SEQ_LEN - 1))
    interp = jnp.maximum(0.0, 1.0 - jnp.abs(pos_frac[:, None] - jnp.arange(N_ANCHORS, dtype=jnp.float32)[None, :]))

    def draw_seq(seq_idx):
        noise_key, anchor_key, pe_key = jax.random.split(jax.random.fold_in(cache_key, seq_idx), 3)
        base_noise = jax.random.normal(noise_key, (SEQ_LEN, KV_LORA), jnp.float32)
        anchors = jax.random.normal(anchor_key, (N_ANCHORS, KV_LORA), jnp.float32)
        latent = 0.8 * base_noise + 0.6 * jnp.dot(interp, anchors)
        rope_part = 1.5 * jax.random.normal(pe_key, (SEQ_LEN, ROPE_DIM), jnp.float32)
        return latent.astype(jnp.bfloat16), rope_part.astype(jnp.bfloat16)

    ckv_cache, kpe_cache = lax.map(draw_seq, jnp.arange(N_SEQS))
    long_key, short_key = jax.random.split(len_key)
    long_len = SEQ_LEN - 1 - jax.random.randint(long_key, (N_SEQS,), 0, SHARD_LEN)
    short_len = jax.random.randint(short_key, (N_SEQS,), SEQ_LEN // 2, SEQ_LEN)
    cache_len = jnp.where(jnp.arange(N_SEQS) % 2 == 0, long_len, short_len).astype(jnp.int32)

    def normal_weight(key_in, arr_shape, fan_in, gain_mul):
        return (jax.random.normal(key_in, arr_shape, jnp.float32) * (gain_mul * fan_in ** -0.5)).astype(jnp.bfloat16)

    hidden = jax.random.normal(hid_key, (N_SEQS, D_MODEL), jnp.float32).astype(jnp.bfloat16)
    return {
        'hidden': hidden,
        'ckv_cache': ckv_cache,
        'kpe_cache': kpe_cache,
        'cache_len': cache_len,
        'w_dq': normal_weight(shared[0], (D_MODEL, Q_LORA), D_MODEL, 1.0),
        'q_gain': jax.random.uniform(shared[1], (Q_LORA,), jnp.float32, minval=0.5, maxval=1.5).astype(jnp.bfloat16),
        'w_uq': normal_weight(shared[2], (Q_LORA, N_HEADS * QK_DIM), Q_LORA, 1.0),
        'w_dkv': normal_weight(shared[3], (D_MODEL, KV_LORA + ROPE_DIM), D_MODEL, 1.0),
        'kv_gain': jax.random.uniform(shared[4], (KV_LORA,), jnp.float32, minval=0.5, maxval=1.5).astype(jnp.bfloat16),
        'w_uk': normal_weight(shared[5], (N_HEADS, NOPE_DIM, KV_LORA), NOPE_DIM, 1.0),
        'w_uv': normal_weight(shared[6], (N_HEADS, V_DIM, KV_LORA), KV_LORA, 5.0),
        'w_out': normal_weight(shared[7], (N_HEADS * V_DIM, D_MODEL), N_HEADS * V_DIM, 1.0),
    }


def reference(hidden, ckv_cache, kpe_cache, cache_len, w_dq, q_gain, w_uq, w_dkv, kv_gain, w_uk, w_uv, w_out):
    score_scale = QK_DIM ** -0.5
    cq_raw = jnp.dot(hidden, w_dq, preferred_element_type=jnp.float32)
    c_q = rms_norm(cq_raw, q_gain).astype(jnp.bfloat16)
    q_full = jnp.dot(c_q, w_uq, preferred_element_type=jnp.float32).astype(jnp.bfloat16)
    q_full = q_full.reshape(N_SEQS, N_HEADS, QK_DIM)
    cos_t, sin_t = rope_tables(cache_len)
    q_pe = rotate(q_full[:, :, NOPE_DIM:].astype(jnp.float32), cos_t[:, None, :], sin_t[:, None, :]).astype(jnp.bfloat16)
    q_lat = jnp.einsum('bhn,hnc->bhc', q_full[:, :, :NOPE_DIM].astype(jnp.float32), w_uk.astype(jnp.float32)).astype(jnp.bfloat16)
    kv_raw = jnp.dot(hidden, w_dkv, preferred_element_type=jnp.float32)
    c_kv = rms_norm(kv_raw[:, :KV_LORA], kv_gain).astype(jnp.bfloat16)
    k_pe = rotate(kv_raw[:, KV_LORA:], cos_t, sin_t).astype(jnp.bfloat16)
    positions = jnp.arange(SEQ_LEN, dtype=jnp.int32)
    new_slot = (positions[None, :] == cache_len[:, None])[:, :, None]
    ckv_out = jnp.where(new_slot, c_kv[:, None, :], ckv_cache)
    kpe_out = jnp.where(new_slot, k_pe[:, None, :], kpe_cache)

    def attend_one(seq_args):
        q_lat_b, q_pe_b, ckv_b, kpe_b, len_b = seq_args
        ckv_f = ckv_b.astype(jnp.float32)
        scores = jnp.einsum('hc,tc->ht', q_lat_b.astype(jnp.float32), ckv_f) + jnp.einsum('hr,tr->ht', q_pe_b.astype(jnp.float32), kpe_b.astype(jnp.float32))
        scores = jnp.where(positions[None, :] <= len_b, scores * score_scale, -jnp.inf)
        attn_probs = jax.nn.softmax(scores, axis=-1)
        return jnp.einsum('ht,tc->hc', attn_probs, ckv_f)

    o_lat = lax.map(attend_one, (q_lat, q_pe, ckv_out, kpe_out, cache_len)).astype(jnp.bfloat16)
    o_heads = jnp.einsum('bhc,hvc->bhv', o_lat.astype(jnp.float32), w_uv.astype(jnp.float32)).astype(jnp.bfloat16)
    out = jnp.dot(o_heads.reshape(N_SEQS, N_HEADS * V_DIM), w_out, preferred_element_type=jnp.float32).astype(jnp.bfloat16)
    kv_new = jnp.concatenate([c_kv, k_pe], axis=-1)
    return (out, ckv_out, kpe_out, kv_new)
```

```python
import functools

import jax
import jax.numpy as jnp
from jax import lax
from jax.experimental import pallas as pl
from jax.experimental.pallas import tpu as pltpu
from jax.sharding import PartitionSpec as P

EPS = 1e-6
ROPE_THETA = 10000.0
NEG_FILL = -1e30
MESH = pl.DeviceIdType.MESH
NBUF = 6
AHEAD = 3
TILE_T = 512
CHUNK = 4


def rms_norm(vector, norm_gain):
    mean_sq = jnp.mean(vector * vector, axis=-1, keepdims=True)
    return vector * lax.rsqrt(mean_sq + EPS) * norm_gain.astype(jnp.float32)


def rope_tables(cache_len, rope_dim):
    inv_freq = jnp.power(ROPE_THETA, -2.0 * jnp.arange(rope_dim // 2, dtype=jnp.float32) / rope_dim)
    rope_angle = cache_len.astype(jnp.float32)[:, None] * inv_freq[None, :]
    return jnp.cos(rope_angle), jnp.sin(rope_angle)


def rotate(vector, cos_t, sin_t):
    half_dim = vector.shape[-1] // 2
    first_half = vector[..., :half_dim]
    second_half = vector[..., half_dim:]
    return jnp.concatenate([first_half * cos_t - second_half * sin_t, second_half * cos_t + first_half * sin_t], axis=-1)


def attend_kernel(n_seqs, shard_len, scale, len_ref, info_ref, qm_ref, qo_ref, pm_ref, po_ref, cnew_ref, knew_ref,
                  ckv_hbm, kpe_hbm, ckv_out, kpe_out, o_ref, lse_ref, cbuf, kbuf, s_scr, lse_scr, in_sem, out_sem):
    step = pl.program_id(0)
    chip = info_ref[1]

    def copies_in(seq):
        slot = lax.rem(seq, NBUF)
        return (pltpu.make_async_copy(ckv_hbm.at[seq], cbuf.at[slot], in_sem.at[0, slot]),
                pltpu.make_async_copy(kpe_hbm.at[seq], kbuf.at[slot], in_sem.at[1, slot]))

    def copies_out(seq):
        slot = lax.rem(seq, NBUF)
        return (pltpu.make_async_copy(cbuf.at[slot], ckv_out.at[seq], out_sem.at[0, slot]),
                pltpu.make_async_copy(kbuf.at[slot], kpe_out.at[seq], out_sem.at[1, slot]))

    @pl.when(step == 0)
    def _():
        for seq in range(AHEAD):
            for copy in copies_in(jnp.int32(seq)):
                copy.start()

    ahead = step + AHEAD

    @pl.when(ahead < n_seqs)
    def _():
        @pl.when(ahead >= NBUF)
        def _():
            for copy in copies_out(ahead - NBUF):
                copy.wait()
        for copy in copies_in(ahead):
            copy.start()

    for copy in copies_in(step):
        copy.wait()
    slot = lax.rem(step, NBUF)
    pos = len_ref[step] - info_ref[0]

    @pl.when((pos >= 0) & (pos < shard_len))
    def _():
        row0 = pl.multiple_of((pos // 16) * 16, 16)
        block = cbuf[slot, pl.ds(row0, 16), :].astype(jnp.float32)
        rows = lax.broadcasted_iota(jnp.int32, block.shape, 0) + row0
        cbuf[slot, pl.ds(row0, 16), :] = jnp.where(rows == pos, cnew_ref[pl.ds(step, 1), :], block).astype(jnp.bfloat16)
        col0 = pl.multiple_of((pos // 128) * 128, 128)
        seq_lane = lax.broadcasted_iota(jnp.int32, knew_ref.shape, 1) == step
        new_col = jnp.sum(jnp.where(seq_lane, knew_ref[...], 0.0), axis=1, keepdims=True)
        kblock = kbuf[slot, :, pl.ds(col0, 128)].astype(jnp.float32)
        cols = lax.broadcasted_iota(jnp.int32, kblock.shape, 1) + col0
        kbuf[slot, :, pl.ds(col0, 128)] = jnp.where(cols == pos, new_col, kblock).astype(jnp.bfloat16)

    q_lat = jnp.concatenate([qm_ref[0], qo_ref[0]], axis=0)
    q_pe = jnp.concatenate([pm_ref[0], po_ref[0]], axis=0)
    peak = None
    for t0 in range(0, shard_len, TILE_T):
        s = lax.dot_general(q_lat, cbuf[slot, t0:t0 + TILE_T, :], (((1,), (1,)), ((), ())), preferred_element_type=jnp.float32)
        s = s + lax.dot_general(q_pe, kbuf[slot, :, t0:t0 + TILE_T], (((1,), (0,)), ((), ())), preferred_element_type=jnp.float32)
        cols = lax.broadcasted_iota(jnp.int32, s.shape, 1) + t0
        s = jnp.where(cols <= pos, s * scale, NEG_FILL)
        s_scr[:, t0:t0 + TILE_T] = s
        tile_peak = jnp.max(s, axis=1, keepdims=True)
        peak = tile_peak if peak is None else jnp.maximum(peak, tile_peak)
    denom = jnp.zeros_like(peak)
    acc = None
    for t0 in range(0, shard_len, TILE_T):
        w = jnp.exp(s_scr[:, t0:t0 + TILE_T] - peak)
        denom = denom + jnp.sum(w, axis=1, keepdims=True)
        part = jnp.dot(w.astype(jnp.bfloat16), cbuf[slot, t0:t0 + TILE_T, :], preferred_element_type=jnp.float32)
        acc = part if acc is None else acc + part
    for copy in copies_out(step):
        copy.start()
    o = acc * (1.0 / denom)
    for half in range(2):
        for group in range(4):
            r0 = half * 64 + group * 16
            o_ref[half, group ^ chip, 0] = o[r0:r0 + 16, :]
    lanes = lax.broadcasted_iota(jnp.int32, lse_scr.shape, 1)
    lse_scr[...] = jnp.where(lanes == step, peak + jnp.log(denom), lse_scr[...])

    @pl.when(step == n_seqs - 1)
    def _():
        lse_ref[...] = jnp.transpose(lse_scr[...])[:n_seqs, :]
        for seq in range(n_seqs - NBUF, n_seqs):
            for copy in copies_out(jnp.int32(seq)):
                copy.wait()


def attend(cache_len, info, q_mine, q_other, pe_mine, pe_other, c_new, k_new, ckv, kpe_t, scale):
    n_seqs, shard_len, lat = ckv.shape
    rope = kpe_t.shape[1]
    per_seq = lambda rows, width: pl.BlockSpec((1, rows, width), lambda i, *_: (i, 0, 0))
    whole = lambda shape: pl.BlockSpec(shape, lambda i, *_: (0,) * len(shape))
    hbm = pl.BlockSpec(memory_space=pl.ANY)
    return pl.pallas_call(
        functools.partial(attend_kernel, n_seqs, shard_len, scale),
        grid_spec=pltpu.PrefetchScalarGridSpec(
            num_scalar_prefetch=2,
            grid=(n_seqs,),
            in_specs=[per_seq(64, lat), per_seq(64, lat), per_seq(64, rope), per_seq(64, rope), whole((n_seqs, lat)),
                      whole((rope, n_seqs)), hbm, hbm],
            out_specs=[hbm, hbm, pl.BlockSpec((2, 4, 1, 16, lat), lambda i, *_: (0, 0, i, 0, 0)), whole((n_seqs, 128))],
            scratch_shapes=[
                pltpu.VMEM((NBUF, shard_len, lat), jnp.bfloat16),
                pltpu.VMEM((NBUF, rope, shard_len), jnp.bfloat16),
                pltpu.VMEM((128, shard_len), jnp.float32),
                pltpu.VMEM((128, 128), jnp.float32),
                pltpu.SemaphoreType.DMA((2, NBUF)),
                pltpu.SemaphoreType.DMA((2, NBUF)),
            ],
        ),
        out_shape=[
            jax.ShapeDtypeStruct(ckv.shape, ckv.dtype),
            jax.ShapeDtypeStruct(kpe_t.shape, kpe_t.dtype),
            jax.ShapeDtypeStruct((2, 4, n_seqs, 16, lat), jnp.float32),
            jax.ShapeDtypeStruct((n_seqs, 128), jnp.float32),
        ],
        compiler_params=pltpu.CompilerParams(dimension_semantics=("arbitrary",), vmem_limit_bytes=60 * 1024 * 1024),
        name="attend",
    )(cache_len, info, q_mine, q_other, pe_mine, pe_other, c_new, k_new, ckv, kpe_t)


def combine_kernel(n_seqs, o_hbm, lse_ref, wuv_hbm, wout_hbm, out_ref, mine, got1, got2, got3, lse_all, w_mine, w_part,
                   wuv, wout, heads, part, part_got, quad, full, load_sem, wt_sem, d1_s, d1_r, s2_s, s2_r, s3_s, s3_r,
                   l_s, l_r, a_s, a_r, b_s, b_r, c_s, c_r, e_s, e_r):
    me = lax.axis_index("sp")
    core = lax.rem(me, 2)
    x_bit = lax.rem(me // 2, 2)
    y_bit = me // 4
    chip = me // 2

    def flip(bits):
        dev = me
        if bits & 1:
            dev = dev + 1 - 2 * core
        if bits & 2:
            dev = dev + 2 - 4 * x_bit
        if bits & 4:
            dev = dev + 4 - 8 * y_bit
        return dev

    def send(src, dst, ssem, rsem, bits):
        return pltpu.make_async_remote_copy(src_ref=src, dst_ref=dst, send_sem=ssem, recv_sem=rsem,
                                            device_id={"sp": flip(bits)}, device_id_type=MESH)

    head0 = core * 64 + chip * 16
    wuv_copy = pltpu.make_async_copy(wuv_hbm.at[pl.ds(head0, 16)], wuv, wt_sem.at[0])
    wout_copy = pltpu.make_async_copy(wout_hbm.at[pl.ds(pl.multiple_of(head0 * 128, 2048), 2048)], wout, wt_sem.at[1])
    n_chunks = n_seqs // CHUNK
    loads = []
    for c in range(n_chunks):
        seqs = pl.ds(c * CHUNK, CHUNK)
        loads.append(pltpu.make_async_copy(o_hbm.at[0, :, seqs], mine.at[:, seqs], load_sem.at[c]))
        loads[c].start()
    wuv_copy.start()
    wout_copy.start()

    barrier = pltpu.get_barrier_semaphore()
    for bits in range(1, 8):
        pl.semaphore_signal(barrier, inc=1, device_id={"sp": flip(bits)}, device_id_type=MESH)
    pl.semaphore_wait(barrier, 7)

    lse_sends = [send(lse_ref, lse_all.at[bits], l_s.at[bits], l_r.at[bits], bits) for bits in range(1, 8)]
    for copy in lse_sends:
        copy.start()
    d1 = []
    for c in range(n_chunks):
        seqs = pl.ds(c * CHUNK, CHUNK)
        d1.append(send(o_hbm.at[1, :, seqs], got1.at[:, seqs], d1_s.at[c], d1_r.at[c], 1))
        d1[c].start()

    for copy in lse_sends:
        copy.wait_recv()
    lses = [lse_ref[...]]
    for bits in range(1, 8):
        other = lse_all[bits]
        lses.append(pltpu.roll(other, 64, 1) if bits & 1 else other)
    peak = functools.reduce(jnp.maximum, lses)
    total = functools.reduce(jnp.add, [jnp.exp(v - peak) for v in lses])
    norm = peak + jnp.log(total)
    pad = jnp.zeros((128 - n_seqs, 128), jnp.float32)
    for value, dst in ((lses[0], w_mine), (lses[1], w_part)):
        wt = jnp.transpose(jnp.concatenate([jnp.exp(value - norm), pad], axis=0))[:64, :]
        for s in range(n_seqs):
            dst[s] = jnp.broadcast_to(wt[:, s:s + 1], (64, 128))

    def orders(c):
        return (1, 2) if c % 2 == 0 else (2, 1)

    s2 = []
    for c in range(n_chunks):
        loads[c].wait()
        d1[c].wait_recv()
        for j in range(4):
            flip_x = x_bit + (1 - 2 * x_bit if j & 1 else 0)
            flip_y = y_bit + (1 - 2 * y_bit if j & 2 else 0)
            row0 = pl.multiple_of((flip_y * 2 + flip_x) * 16, 16)

            def merge(i, _, j=j, row0=row0, c=c):
                s = c * CHUNK + i
                wa = w_mine[s, pl.ds(row0, 16), :]
                wb = w_part[s, pl.ds(row0, 16), :]
                wa = jnp.concatenate([wa] * 4, axis=1)
                wb = jnp.concatenate([wb] * 4, axis=1)
                mine[j, s] = mine[j, s] * wa + got1[j, s] * wb
                return 0

            lax.fori_loop(0, CHUNK, merge, 0)
        first, _ = orders(c)
        seqs = pl.ds(c * CHUNK, CHUNK)
        s2.append((send(mine.at[first, seqs], got2.at[0, seqs], s2_s.at[0, c], s2_r.at[0, c], 2 * first),
                   send(mine.at[3, seqs], got2.at[1, seqs], s2_s.at[1, c], s2_r.at[1, c], 2 * first)))
        for copy in s2[c]:
            copy.start()

    s3 = []
    for c in range(n_chunks):
        _, second = orders(c)
        s2[c][0].wait_recv()
        s2[c][1].wait_recv()

        def add2(i, _, second=second, c=c):
            s = c * CHUNK + i
            mine[second, s] = mine[second, s] + got2[1, s]
            mine[0, s] = mine[0, s] + got2[0, s]
            return 0

        lax.fori_loop(0, CHUNK, add2, 0)
        seqs = pl.ds(c * CHUNK, CHUNK)
        s3.append(send(mine.at[second, seqs], got3.at[seqs], s3_s.at[c], s3_r.at[c], 2 * second))
        s3[c].start()

    for c in range(n_chunks):
        s3[c].wait_recv()

        def add3(i, _, c=c):
            s = c * CHUNK + i
            mine[0, s] = mine[0, s] + got3[s]
            return 0

        lax.fori_loop(0, CHUNK, add3, 0)

    wuv_copy.wait()
    for h in range(16):
        x = mine[0, :, h, :].astype(jnp.bfloat16)
        o = lax.dot_general(x, wuv[h], (((1,), (1,)), ((), ())), preferred_element_type=jnp.float32)
        heads[:, h * 128:(h + 1) * 128] = o.astype(jnp.bfloat16)
    wout_copy.wait()
    width = wout.shape[1] // 8

    for p in range(8):
        part[p // 4, p % 4] = jnp.dot(heads[...], wout[:, p * width:(p + 1) * width], preferred_element_type=jnp.float32)

    a = send(part.at[1 - core], part_got, a_s, a_r, 1)
    a.start()
    a.wait_recv()
    part[core] = part[core] + part_got[...]
    b = []
    for j in range(1, 4):
        flip_x = x_bit + (1 - 2 * x_bit if j & 1 else 0)
        flip_y = y_bit + (1 - 2 * y_bit if j & 2 else 0)
        b.append(send(part.at[core, flip_y * 2 + flip_x], quad.at[j - 1], b_s.at[j - 1], b_r.at[j - 1], 2 * j))
        b[-1].start()
    for copy in b:
        copy.wait_recv()
    done = part[core, chip] + quad[0] + quad[1] + quad[2]
    full[core, chip] = done.astype(jnp.bfloat16).astype(jnp.float32)
    g = [send(full.at[core, chip], full.at[core, chip], c_s.at[j - 1], c_r.at[j - 1], 2 * j) for j in range(1, 4)]
    for copy in g:
        copy.start()
    for copy in g:
        copy.wait_recv()
    e = send(full.at[core], full.at[core], e_s, e_r, 1)
    e.start()
    e.wait_recv()
    for p in range(8):
        out_ref[:, p * width:(p + 1) * width] = full[p // 4, p % 4].astype(jnp.bfloat16)

    for copy in lse_sends + d1 + [c for pair in s2 for c in pair] + s3 + [a] + b + g + [e]:
        copy.wait_send()


def combine(o_parts, lse, w_uv, w_out):
    _, _, n_seqs, _, lat = o_parts.shape
    d_model = w_out.shape[1]
    vdim = w_uv.shape[1]
    n_chunks = n_seqs // CHUNK
    width = d_model // 8
    hbm = pl.BlockSpec(memory_space=pl.ANY)
    vmem = pl.BlockSpec(memory_space=pltpu.VMEM)
    dma = pltpu.SemaphoreType.DMA
    f32 = jnp.float32
    return pl.pallas_call(
        functools.partial(combine_kernel, n_seqs),
        out_shape=jax.ShapeDtypeStruct((n_seqs, d_model), jnp.bfloat16),
        in_specs=[hbm, vmem, hbm, hbm],
        out_specs=vmem,
        scratch_shapes=[
            pltpu.VMEM((4, n_seqs, 16, lat), f32),
            pltpu.VMEM((4, n_seqs, 16, lat), f32),
            pltpu.VMEM((2, n_seqs, 16, lat), f32),
            pltpu.VMEM((n_seqs, 16, lat), f32),
            pltpu.VMEM((8, n_seqs, 128), f32),
            pltpu.VMEM((n_seqs, 64, 128), f32),
            pltpu.VMEM((n_seqs, 64, 128), f32),
            pltpu.VMEM((16, vdim, lat), jnp.bfloat16),
            pltpu.VMEM((16 * vdim, d_model), jnp.bfloat16),
            pltpu.VMEM((n_seqs, 16 * vdim), jnp.bfloat16),
            pltpu.VMEM((2, 4, n_seqs, width), f32),
            pltpu.VMEM((4, n_seqs, width), f32),
            pltpu.VMEM((3, n_seqs, width), f32),
            pltpu.VMEM((2, 4, n_seqs, width), f32),
            dma((n_chunks,)), dma((2,)),
            dma((n_chunks,)), dma((n_chunks,)),
            dma((2, n_chunks)), dma((2, n_chunks)),
            dma((n_chunks,)), dma((n_chunks,)),
            dma((8,)), dma((8,)),
            dma, dma, dma((3,)), dma((3,)), dma((3,)), dma((3,)), dma, dma,
        ],
        compiler_params=pltpu.CompilerParams(collective_id=0, has_side_effects=True, vmem_limit_bytes=60 * 1024 * 1024),
        name="combine",
    )(o_parts, lse, w_uv, w_out)


def solution(mesh):
    def local_step(hidden, ckv_blk, kpe_blk, cache_len, w_dq, q_gain, w_uq, w_dkv, kv_gain, w_uk, w_uv, w_out):
        n_seqs = hidden.shape[0]
        shard_len, lat = ckv_blk.shape[1:]
        n_heads, nope, _ = w_uk.shape
        qk_dim = w_uq.shape[1] // n_heads
        half = n_heads // 2
        scale = (nope + kpe_blk.shape[2]) ** -0.5
        me = lax.axis_index("sp")
        core = me % 2
        cq_raw = jnp.dot(hidden, w_dq, preferred_element_type=jnp.float32)
        c_q = rms_norm(cq_raw, q_gain).astype(jnp.bfloat16)
        w_half = lax.dynamic_slice(w_uq, (0, core * half * qk_dim), (w_uq.shape[0], half * qk_dim))
        q_mine = jnp.dot(c_q, w_half, preferred_element_type=jnp.float32).astype(jnp.bfloat16)
        q_other = lax.ppermute(q_mine.astype(jnp.float32), "sp", [(i, i ^ 1) for i in range(8)])
        cos_t, sin_t = rope_tables(cache_len, qk_dim - nope)

        def finish(q_part, which):
            q_part = q_part.astype(jnp.float32).reshape(n_seqs, half, qk_dim)
            q_pe = rotate(q_part[:, :, nope:], cos_t[:, None, :], sin_t[:, None, :]).astype(jnp.bfloat16)
            uk = lax.dynamic_slice(w_uk, (which * half, 0, 0), (half, nope, lat))
            q_lat = jnp.einsum("bhn,hnc->bhc", q_part[:, :, :nope].astype(jnp.bfloat16), uk, preferred_element_type=jnp.float32)
            return q_lat.astype(jnp.bfloat16), q_pe

        lat_mine, pe_mine = finish(q_mine, core)
        lat_other, pe_other = finish(q_other, 1 - core)
        kv_raw = jnp.dot(hidden, w_dkv, preferred_element_type=jnp.float32)
        c_kv = rms_norm(kv_raw[:, :lat], kv_gain)
        k_pe = rotate(kv_raw[:, lat:], cos_t, sin_t)
        kv_new = jnp.concatenate([c_kv, k_pe], axis=-1).astype(jnp.bfloat16)
        kv_new_f = kv_new.astype(jnp.float32)
        info = jnp.stack([me * shard_len, me // 2]).astype(jnp.int32)
        ckv_out, kpe_out, o_parts, lse = attend(cache_len, info, lat_mine, lat_other, pe_mine, pe_other, kv_new_f[:, :lat],
                                                kv_new_f[:, lat:].T, ckv_blk, jnp.swapaxes(kpe_blk, 1, 2), scale)
        out = combine(o_parts, lse, w_uv, w_out)
        return out, ckv_out, jnp.swapaxes(kpe_out, 1, 2), kv_new

    cache_spec = P("dp", "sp", None)
    return jax.shard_map(local_step, mesh=mesh, in_specs=(P("dp", None), cache_spec, cache_spec, P("dp"), P(), P(), P(), P(), P(), P(), P(), P()), out_specs=(P("dp", None), cache_spec, cache_spec, P("dp", None)), check_vma=False)
```

```python
import functools

import jax
import jax.numpy as jnp
from jax import lax
from jax.experimental import pallas as pl
from jax.experimental.pallas import tpu as pltpu
from jax.sharding import PartitionSpec as P

EPS = 1e-6
ROPE_THETA = 10000.0
NEG_FILL = -1e30
MESH = pl.DeviceIdType.MESH
NBUF = 20
AHEAD = 10
TILE_T = 512
CHUNK = 4


def rope_tables(cache_len, rope_dim):
    inv_freq = jnp.power(ROPE_THETA, -2.0 * jnp.arange(rope_dim // 2, dtype=jnp.float32) / rope_dim)
    rope_angle = cache_len.astype(jnp.float32)[:, None] * inv_freq[None, :]
    return jnp.cos(rope_angle), jnp.sin(rope_angle)


def project_kernel(n_seqs, hid_ref, qg_ref, kvg_ref, cos_ref, sin_ref, wdq_hbm, wdkv_hbm, wuq_hbm, wuk_hbm,
                   lat_hbm, pe_hbm, kv_ref, cnew_ref, knew_ref, dq_buf, dkv_buf, uq_buf, uk_buf, q_mine, q_other,
                   lat_scr, pe_scr, lat_out, pe_out, dq_sem, dkv_sem, uq_sem, uk_sem, lo_sem, po_sem, q_s, q_r):
    core = lax.rem(lax.axis_index("sp"), 2)
    partner = lax.axis_index("sp") + 1 - 2 * core
    f32, bf16 = jnp.float32, jnp.bfloat16
    n_dq, rows, q_lora = dq_buf.shape
    tile = uq_buf.shape[2]
    n_tiles = q_mine.shape[0]
    lat = lat_scr.shape[2]
    uq_slots = uq_buf.shape[0]
    uk_slots = uk_buf.shape[0]

    def uq_copy(i):
        slot = lax.rem(i, uq_slots)
        col = pl.multiple_of(core * (n_tiles * tile) + i * tile, tile)
        return pltpu.make_async_copy(wuq_hbm.at[:, pl.ds(col, tile)], uq_buf.at[slot], uq_sem.at[slot])

    def uk_copy(i):
        half = i // 4
        head = (core + half - 2 * core * half) * 64 + lax.rem(i, 4) * 16
        slot = lax.rem(i, uk_slots)
        return pltpu.make_async_copy(wuk_hbm.at[pl.ds(head, 16)], uk_buf.at[slot], uk_sem.at[slot])

    dq_copies = [pltpu.make_async_copy(wdq_hbm.at[pl.ds(i * rows, rows)], dq_buf.at[i], dq_sem.at[i]) for i in range(n_dq)]
    dkv_copy = pltpu.make_async_copy(wdkv_hbm, dkv_buf, dkv_sem)
    for copy in dq_copies:
        copy.start()
    for i in range(uq_slots):
        uq_copy(jnp.int32(i)).start()
    dkv_copy.start()

    barrier = pltpu.get_barrier_semaphore()
    pl.semaphore_signal(barrier, inc=1, device_id={"sp": partner}, device_id_type=MESH)
    pl.semaphore_wait(barrier, 1)

    def norm(v, gain):
        mean_sq = jnp.mean(v * v, axis=-1, keepdims=True)
        return v * lax.rsqrt(mean_sq + EPS) * gain.astype(f32)

    acc = jnp.zeros((n_seqs, q_lora), f32)
    for i in range(n_dq):
        dq_copies[i].wait()
        acc = acc + jnp.dot(hid_ref[:, i * rows:(i + 1) * rows], dq_buf[i], preferred_element_type=f32)
    c_q = norm(acc, qg_ref[...]).astype(bf16)

    def q_send(i):
        return pltpu.make_async_remote_copy(src_ref=q_mine.at[i], dst_ref=q_other.at[i], send_sem=q_s.at[i], recv_sem=q_r.at[i],
                                            device_id={"sp": partner}, device_id_type=MESH)

    def q_tile(i, _):
        uq_copy(i).wait()
        q = jnp.dot(c_q, uq_buf[lax.rem(i, uq_slots)], preferred_element_type=f32)
        q_mine[i] = q.astype(bf16).astype(f32)

        @pl.when(i + uq_slots < n_tiles)
        def _():
            uq_copy(i + uq_slots).start()

        @pl.when(i == n_tiles - uq_slots)
        def _():
            for k in range(uk_slots):
                uk_copy(jnp.int32(k)).start()

        @pl.when(i > 0)
        def _():
            q_send(i - 1).start()
        return 0

    lax.fori_loop(0, n_tiles, q_tile, 0)
    cos_t, sin_t = cos_ref[...], sin_ref[...]
    lane = lax.broadcasted_iota(jnp.int32, (n_seqs, 128), 1)
    low_half = lax.rem(lane, 64) < 32

    def rotate_pairs(x):
        swapped = jnp.where(low_half, pltpu.roll(x, 96, 1), pltpu.roll(x, 32, 1))
        return x * cos_t + swapped * sin_t

    dkv_copy.wait()
    kv = lax.dot_general(hid_ref[...], dkv_buf[...], (((1,), (1,)), ((), ())), preferred_element_type=f32)
    q_send(jnp.int32(n_tiles - 1)).start()
    c_kv = norm(kv[:, :lat], kvg_ref[...]).astype(bf16)
    k_raw = jnp.concatenate([kv[:, lat:], jnp.zeros((n_seqs, 64), f32)], axis=1)
    k_pe = rotate_pairs(k_raw).astype(bf16)
    kv_ref[:, :lat] = c_kv
    kv_ref[:, lat:] = k_pe[:, :64]
    cnew_ref[...] = c_kv.astype(f32)
    square = jnp.concatenate([k_pe.astype(f32), jnp.zeros((128 - n_seqs, 128), f32)], axis=0)
    knew_ref[...] = jnp.transpose(square)[:64, :]

    def out_copies(half, g):
        return (pltpu.make_async_copy(lat_out.at[half, g], lat_hbm.at[half, :, pl.ds(g * 16, 16)], lo_sem.at[half, g]),
                pltpu.make_async_copy(pe_out.at[half, g], pe_hbm.at[half, :, pl.ds(g * 16, 16)], po_sem.at[half, g]))

    for half in range(2):
        src = q_mine if half == 0 else q_other

        def group(g, _, half=half, src=src):
            i = half * 4 + g
            uk_copy(i).wait()
            slot = lax.rem(i, uk_slots)
            if half == 1:
                q_send(2 * g).wait_recv()
                q_send(2 * g + 1).wait_recv()
            for h in range(0, 16, 2):
                t, p = divmod(h // 2, 4)
                v = src[2 * g + t, :, p * 384:(p + 1) * 384]
                even = v[:, :128].astype(bf16)
                odd = pltpu.roll(v, 192, 1)[:, :128].astype(bf16)
                x = jnp.where(lane < 64, v[:, 128:256], v[:, 256:384])
                rot = rotate_pairs(x)
                pe_scr[:, h, :] = rot
                pe_scr[:, h + 1, :] = pltpu.roll(rot, 64, 1)
                lat_scr[:, h, :] = jnp.dot(even, uk_buf[slot, h], preferred_element_type=f32)
                lat_scr[:, h + 1, :] = jnp.dot(odd, uk_buf[slot, h + 1], preferred_element_type=f32)
            lat_out[half, g] = lat_scr[...].astype(bf16)
            pe_out[half, g] = pe_scr[...][:, :, :64].astype(bf16)

            @pl.when(i + uk_slots < 8)
            def _():
                uk_copy(i + uk_slots).start()
            for copy in out_copies(half, g):
                copy.start()
            return 0

        lax.fori_loop(0, 4, group, 0)

    def drain(g, _):
        for half in range(2):
            for copy in out_copies(half, g):
                copy.wait()
        q_send(2 * g).wait_send()
        q_send(2 * g + 1).wait_send()
        return 0

    lax.fori_loop(0, 4, drain, 0)


def project(hidden, cos_t, sin_t, w_dq, q_gain, w_uq, w_dkv_t, kv_gain, w_uk):
    n_seqs, d_model = hidden.shape
    q_lora = w_dq.shape[1]
    n_heads, nope, lat = w_uk.shape
    rope = w_uq.shape[1] // n_heads - nope
    tile = 8 * (nope + rope)
    n_tiles = n_heads // 16
    n_dq, uq_slots, uk_slots = 8, 3, 4
    f32, bf16 = jnp.float32, jnp.bfloat16
    hbm = pl.BlockSpec(memory_space=pl.ANY)
    vmem = pl.BlockSpec(memory_space=pltpu.VMEM)
    dma = pltpu.SemaphoreType.DMA
    return pl.pallas_call(
        functools.partial(project_kernel, n_seqs),
        out_shape=[
            jax.ShapeDtypeStruct((2, n_seqs, 64, lat), bf16),
            jax.ShapeDtypeStruct((2, n_seqs, 64, rope), bf16),
            jax.ShapeDtypeStruct((n_seqs, lat + rope), bf16),
            jax.ShapeDtypeStruct((n_seqs, lat), f32),
            jax.ShapeDtypeStruct((rope, 128), f32),
        ],
        in_specs=[vmem] * 5 + [hbm] * 4,
        out_specs=[hbm, hbm, vmem, vmem, vmem],
        scratch_shapes=[
            pltpu.VMEM((n_dq, d_model // n_dq, q_lora), bf16),
            pltpu.VMEM((lat + rope, d_model), bf16),
            pltpu.VMEM((uq_slots, q_lora, tile), bf16),
            pltpu.VMEM((uk_slots, 16, nope, lat), bf16),
            pltpu.VMEM((n_tiles, n_seqs, tile), f32),
            pltpu.VMEM((n_tiles, n_seqs, tile), f32),
            pltpu.VMEM((n_seqs, 16, lat), f32),
            pltpu.VMEM((n_seqs, 16, 128), f32),
            pltpu.VMEM((2, 4, n_seqs, 16, lat), bf16),
            pltpu.VMEM((2, 4, n_seqs, 16, rope), bf16),
            dma((n_dq,)), dma, dma((uq_slots,)), dma((uk_slots,)), dma((2, 4)), dma((2, 4)), dma((n_tiles,)), dma((n_tiles,)),
        ],
        compiler_params=pltpu.CompilerParams(collective_id=1, has_side_effects=True, vmem_limit_bytes=60 * 1024 * 1024),
        name="project",
    )(hidden, q_gain[None, :], kv_gain[None, :], cos_t, sin_t, w_dq, w_dkv_t, w_uq, w_uk)


def attend_kernel(n_seqs, shard_len, scale, len_ref, info_ref, q_ref, pe_ref, cnew_ref, knew_ref,
                  ckv_hbm, kpe_hbm, ckv_out, kpe_out, o_ref, lse_ref, cbuf, kbuf, s_scr, lse_scr, in_sem, out_sem):
    step = pl.program_id(0)
    chip = info_ref[1]

    def copies_in(seq):
        slot = lax.rem(seq, NBUF)
        return (pltpu.make_async_copy(ckv_hbm.at[seq], cbuf.at[slot], in_sem.at[0, slot]),
                pltpu.make_async_copy(kpe_hbm.at[seq], kbuf.at[slot], in_sem.at[1, slot]))

    def copies_out(seq):
        slot = lax.rem(seq, NBUF)
        return (pltpu.make_async_copy(cbuf.at[slot], ckv_out.at[seq], out_sem.at[0, slot]),
                pltpu.make_async_copy(kbuf.at[slot], kpe_out.at[seq], out_sem.at[1, slot]))

    @pl.when(step == 0)
    def _():
        for seq in range(AHEAD):
            for copy in copies_in(jnp.int32(seq)):
                copy.start()

    ahead = step + AHEAD

    @pl.when(ahead < n_seqs)
    def _():
        @pl.when(ahead >= NBUF)
        def _():
            for copy in copies_out(ahead - NBUF):
                copy.wait()
        for copy in copies_in(ahead):
            copy.start()

    for copy in copies_in(step):
        copy.wait()
    slot = lax.rem(step, NBUF)
    pos = len_ref[step] - info_ref[0]

    @pl.when((pos >= 0) & (pos < shard_len))
    def _():
        row0 = pl.multiple_of((pos // 16) * 16, 16)
        block = cbuf[slot, pl.ds(row0, 16), :].astype(jnp.float32)
        rows = lax.broadcasted_iota(jnp.int32, block.shape, 0) + row0
        cbuf[slot, pl.ds(row0, 16), :] = jnp.where(rows == pos, cnew_ref[pl.ds(step, 1), :], block).astype(jnp.bfloat16)
        col0 = pl.multiple_of((pos // 128) * 128, 128)
        seq_lane = lax.broadcasted_iota(jnp.int32, knew_ref.shape, 1) == step
        new_col = jnp.sum(jnp.where(seq_lane, knew_ref[...], 0.0), axis=1, keepdims=True)
        kblock = kbuf[slot, :, pl.ds(col0, 128)].astype(jnp.float32)
        cols = lax.broadcasted_iota(jnp.int32, kblock.shape, 1) + col0
        kbuf[slot, :, pl.ds(col0, 128)] = jnp.where(cols == pos, new_col, kblock).astype(jnp.bfloat16)

    q_lat = jnp.concatenate([q_ref[0, 0], q_ref[1, 0]], axis=0)
    q_pe = jnp.concatenate([pe_ref[0, 0], pe_ref[1, 0]], axis=0)
    peak = None
    for t0 in range(0, shard_len, TILE_T):
        s = lax.dot_general(q_lat, cbuf[slot, t0:t0 + TILE_T, :], (((1,), (1,)), ((), ())), preferred_element_type=jnp.float32)
        s = s + lax.dot_general(q_pe, kbuf[slot, :, t0:t0 + TILE_T], (((1,), (0,)), ((), ())), preferred_element_type=jnp.float32)
        cols = lax.broadcasted_iota(jnp.int32, s.shape, 1) + t0
        s = jnp.where(cols <= pos, s * scale, NEG_FILL)
        s_scr[:, t0:t0 + TILE_T] = s
        tile_peak = jnp.max(s, axis=1, keepdims=True)
        peak = tile_peak if peak is None else jnp.maximum(peak, tile_peak)
    denom = jnp.zeros_like(peak)
    acc = None
    for t0 in range(0, shard_len, TILE_T):
        w = jnp.exp(s_scr[:, t0:t0 + TILE_T] - peak)
        denom = denom + jnp.sum(w, axis=1, keepdims=True)
        part = jnp.dot(w.astype(jnp.bfloat16), cbuf[slot, t0:t0 + TILE_T, :], preferred_element_type=jnp.float32)
        acc = part if acc is None else acc + part
    for copy in copies_out(step):
        copy.start()
    o = acc * (1.0 / denom)
    for half in range(2):
        for group in range(4):
            r0 = half * 64 + group * 16
            o_ref[half, group ^ chip, 0] = o[r0:r0 + 16, :]
    lanes = lax.broadcasted_iota(jnp.int32, lse_scr.shape, 1)
    lse_scr[...] = jnp.where(lanes == step, peak + jnp.log(denom), lse_scr[...])

    @pl.when(step == n_seqs - 1)
    def _():
        lse_ref[...] = jnp.transpose(lse_scr[...])[:n_seqs, :]
        for seq in range(n_seqs - NBUF, n_seqs):
            for copy in copies_out(jnp.int32(seq)):
                copy.wait()


def attend(cache_len, info, q_lat, q_pe, c_new, k_new, ckv, kpe_t, scale):
    n_seqs, shard_len, lat = ckv.shape
    rope = kpe_t.shape[1]
    per_seq = lambda width: pl.BlockSpec((2, 1, 64, width), lambda i, *_: (0, i, 0, 0))
    whole = lambda shape: pl.BlockSpec(shape, lambda i, *_: (0,) * len(shape))
    hbm = pl.BlockSpec(memory_space=pl.ANY)
    return pl.pallas_call(
        functools.partial(attend_kernel, n_seqs, shard_len, scale),
        grid_spec=pltpu.PrefetchScalarGridSpec(
            num_scalar_prefetch=2,
            grid=(n_seqs,),
            in_specs=[per_seq(lat), per_seq(rope), whole((n_seqs, lat)), whole((rope, 128)), hbm, hbm],
            out_specs=[hbm, hbm, pl.BlockSpec((2, 4, 1, 16, lat), lambda i, *_: (0, 0, i, 0, 0)), whole((n_seqs, 128))],
            scratch_shapes=[
                pltpu.VMEM((NBUF, shard_len, lat), jnp.bfloat16),
                pltpu.VMEM((NBUF, rope, shard_len), jnp.bfloat16),
                pltpu.VMEM((128, shard_len), jnp.float32),
                pltpu.VMEM((128, 128), jnp.float32),
                pltpu.SemaphoreType.DMA((2, NBUF)),
                pltpu.SemaphoreType.DMA((2, NBUF)),
            ],
        ),
        out_shape=[
            jax.ShapeDtypeStruct(ckv.shape, ckv.dtype),
            jax.ShapeDtypeStruct(kpe_t.shape, kpe_t.dtype),
            jax.ShapeDtypeStruct((2, 4, n_seqs, 16, lat), jnp.float32),
            jax.ShapeDtypeStruct((n_seqs, 128), jnp.float32),
        ],
        compiler_params=pltpu.CompilerParams(dimension_semantics=("arbitrary",), vmem_limit_bytes=60 * 1024 * 1024),
        name="attend",
    )(cache_len, info, q_lat, q_pe, c_new, k_new, ckv, kpe_t)


def combine_kernel(n_seqs, o_hbm, lse_ref, wuv_hbm, wout_hbm, out_ref, mine, got1, got2, got3, lse_all, w_mine, w_part,
                   wuv, wout, heads, part, part_got, quad, full, load_sem, wt_sem, d1_s, d1_r, s2_s, s2_r, s3_s, s3_r,
                   l_s, l_r, a_s, a_r, b_s, b_r, c_s, c_r, e_s, e_r):
    me = lax.axis_index("sp")
    core = lax.rem(me, 2)
    x_bit = lax.rem(me // 2, 2)
    y_bit = me // 4
    chip = me // 2

    def flip(bits):
        dev = me
        if bits & 1:
            dev = dev + 1 - 2 * core
        if bits & 2:
            dev = dev + 2 - 4 * x_bit
        if bits & 4:
            dev = dev + 4 - 8 * y_bit
        return dev

    def send(src, dst, ssem, rsem, bits):
        return pltpu.make_async_remote_copy(src_ref=src, dst_ref=dst, send_sem=ssem, recv_sem=rsem,
                                            device_id={"sp": flip(bits)}, device_id_type=MESH)

    head0 = core * 64 + chip * 16
    wuv_copy = pltpu.make_async_copy(wuv_hbm.at[pl.ds(head0, 16)], wuv, wt_sem.at[0])
    wout_copy = pltpu.make_async_copy(wout_hbm.at[pl.ds(pl.multiple_of(head0 * 128, 2048), 2048)], wout, wt_sem.at[1])
    n_chunks = n_seqs // CHUNK
    loads = []
    for c in range(n_chunks):
        seqs = pl.ds(c * CHUNK, CHUNK)
        loads.append(pltpu.make_async_copy(o_hbm.at[0, :, seqs], mine.at[:, seqs], load_sem.at[c]))
        loads[c].start()
    wuv_copy.start()
    wout_copy.start()

    barrier = pltpu.get_barrier_semaphore()
    for bits in range(1, 8):
        pl.semaphore_signal(barrier, inc=1, device_id={"sp": flip(bits)}, device_id_type=MESH)
    pl.semaphore_wait(barrier, 7)

    lse_sends = [send(lse_ref, lse_all.at[bits], l_s.at[bits], l_r.at[bits], bits) for bits in range(1, 8)]
    for copy in lse_sends:
        copy.start()
    d1 = []
    for c in range(n_chunks):
        seqs = pl.ds(c * CHUNK, CHUNK)
        d1.append(send(o_hbm.at[1, :, seqs], got1.at[:, seqs], d1_s.at[c], d1_r.at[c], 1))
        d1[c].start()

    for copy in lse_sends:
        copy.wait_recv()
    lses = [lse_ref[...]]
    for bits in range(1, 8):
        other = lse_all[bits]
        lses.append(pltpu.roll(other, 64, 1) if bits & 1 else other)
    peak = functools.reduce(jnp.maximum, lses)
    total = functools.reduce(jnp.add, [jnp.exp(v - peak) for v in lses])
    norm = peak + jnp.log(total)
    pad = jnp.zeros((128 - n_seqs, 128), jnp.float32)
    for value, dst in ((lses[0], w_mine), (lses[1], w_part)):
        wt = jnp.transpose(jnp.concatenate([jnp.exp(value - norm), pad], axis=0))[:64, :]
        for s in range(n_seqs):
            dst[s] = jnp.broadcast_to(wt[:, s:s + 1], (64, 128))

    def orders(c):
        return (1, 2) if c % 2 == 0 else (2, 1)

    s2 = []
    for c in range(n_chunks):
        loads[c].wait()
        d1[c].wait_recv()
        for j in range(4):
            flip_x = x_bit + (1 - 2 * x_bit if j & 1 else 0)
            flip_y = y_bit + (1 - 2 * y_bit if j & 2 else 0)
            row0 = pl.multiple_of((flip_y * 2 + flip_x) * 16, 16)

            def merge(i, _, j=j, row0=row0, c=c):
                s = c * CHUNK + i
                wa = w_mine[s, pl.ds(row0, 16), :]
                wb = w_part[s, pl.ds(row0, 16), :]
                wa = jnp.concatenate([wa] * 4, axis=1)
                wb = jnp.concatenate([wb] * 4, axis=1)
                mine[j, s] = mine[j, s] * wa + got1[j, s] * wb
                return 0

            lax.fori_loop(0, CHUNK, merge, 0)
        first, _ = orders(c)
        seqs = pl.ds(c * CHUNK, CHUNK)
        s2.append((send(mine.at[first, seqs], got2.at[0, seqs], s2_s.at[0, c], s2_r.at[0, c], 2 * first),
                   send(mine.at[3, seqs], got2.at[1, seqs], s2_s.at[1, c], s2_r.at[1, c], 2 * first)))
        for copy in s2[c]:
            copy.start()

    s3 = []
    for c in range(n_chunks):
        _, second = orders(c)
        s2[c][0].wait_recv()
        s2[c][1].wait_recv()

        def add2(i, _, second=second, c=c):
            s = c * CHUNK + i
            mine[second, s] = mine[second, s] + got2[1, s]
            mine[0, s] = mine[0, s] + got2[0, s]
            return 0

        lax.fori_loop(0, CHUNK, add2, 0)
        seqs = pl.ds(c * CHUNK, CHUNK)
        s3.append(send(mine.at[second, seqs], got3.at[seqs], s3_s.at[c], s3_r.at[c], 2 * second))
        s3[c].start()

    for c in range(n_chunks):
        s3[c].wait_recv()

        def add3(i, _, c=c):
            s = c * CHUNK + i
            mine[0, s] = mine[0, s] + got3[s]
            return 0

        lax.fori_loop(0, CHUNK, add3, 0)

    wuv_copy.wait()
    for h in range(16):
        x = mine[0, :, h, :].astype(jnp.bfloat16)
        o = lax.dot_general(x, wuv[h], (((1,), (1,)), ((), ())), preferred_element_type=jnp.float32)
        heads[:, h * 128:(h + 1) * 128] = o.astype(jnp.bfloat16)
    wout_copy.wait()
    width = wout.shape[1] // 8

    for p in range(8):
        part[p // 4, p % 4] = jnp.dot(heads[...], wout[:, p * width:(p + 1) * width], preferred_element_type=jnp.float32)

    a = send(part.at[1 - core], part_got, a_s, a_r, 1)
    a.start()
    a.wait_recv()
    part[core] = part[core] + part_got[...]
    b = []
    for j in range(1, 4):
        flip_x = x_bit + (1 - 2 * x_bit if j & 1 else 0)
        flip_y = y_bit + (1 - 2 * y_bit if j & 2 else 0)
        b.append(send(part.at[core, flip_y * 2 + flip_x], quad.at[j - 1], b_s.at[j - 1], b_r.at[j - 1], 2 * j))
        b[-1].start()
    for copy in b:
        copy.wait_recv()
    done = part[core, chip] + quad[0] + quad[1] + quad[2]
    full[core, chip] = done.astype(jnp.bfloat16).astype(jnp.float32)
    g = [send(full.at[core, chip], full.at[core, chip], c_s.at[j - 1], c_r.at[j - 1], 2 * j) for j in range(1, 4)]
    for copy in g:
        copy.start()
    for copy in g:
        copy.wait_recv()
    e = send(full.at[core], full.at[core], e_s, e_r, 1)
    e.start()
    e.wait_recv()
    for p in range(8):
        out_ref[:, p * width:(p + 1) * width] = full[p // 4, p % 4].astype(jnp.bfloat16)

    for copy in lse_sends + d1 + [c for pair in s2 for c in pair] + s3 + [a] + b + g + [e]:
        copy.wait_send()


def combine(o_parts, lse, w_uv, w_out):
    _, _, n_seqs, _, lat = o_parts.shape
    d_model = w_out.shape[1]
    vdim = w_uv.shape[1]
    n_chunks = n_seqs // CHUNK
    width = d_model // 8
    hbm = pl.BlockSpec(memory_space=pl.ANY)
    vmem = pl.BlockSpec(memory_space=pltpu.VMEM)
    dma = pltpu.SemaphoreType.DMA
    f32 = jnp.float32
    return pl.pallas_call(
        functools.partial(combine_kernel, n_seqs),
        out_shape=jax.ShapeDtypeStruct((n_seqs, d_model), jnp.bfloat16),
        in_specs=[hbm, vmem, hbm, hbm],
        out_specs=vmem,
        scratch_shapes=[
            pltpu.VMEM((4, n_seqs, 16, lat), f32),
            pltpu.VMEM((4, n_seqs, 16, lat), f32),
            pltpu.VMEM((2, n_seqs, 16, lat), f32),
            pltpu.VMEM((n_seqs, 16, lat), f32),
            pltpu.VMEM((8, n_seqs, 128), f32),
            pltpu.VMEM((n_seqs, 64, 128), f32),
            pltpu.VMEM((n_seqs, 64, 128), f32),
            pltpu.VMEM((16, vdim, lat), jnp.bfloat16),
            pltpu.VMEM((16 * vdim, d_model), jnp.bfloat16),
            pltpu.VMEM((n_seqs, 16 * vdim), jnp.bfloat16),
            pltpu.VMEM((2, 4, n_seqs, width), f32),
            pltpu.VMEM((4, n_seqs, width), f32),
            pltpu.VMEM((3, n_seqs, width), f32),
            pltpu.VMEM((2, 4, n_seqs, width), f32),
            dma((n_chunks,)), dma((2,)),
            dma((n_chunks,)), dma((n_chunks,)),
            dma((2, n_chunks)), dma((2, n_chunks)),
            dma((n_chunks,)), dma((n_chunks,)),
            dma((8,)), dma((8,)),
            dma, dma, dma((3,)), dma((3,)), dma((3,)), dma((3,)), dma, dma,
        ],
        compiler_params=pltpu.CompilerParams(collective_id=0, has_side_effects=True, vmem_limit_bytes=60 * 1024 * 1024),
        name="combine",
    )(o_parts, lse, w_uv, w_out)


def solution(mesh):
    def local_step(hidden, ckv_blk, kpe_blk, cache_len, w_dq, q_gain, w_uq, w_dkv, kv_gain, w_uk, w_uv, w_out):
        shard_len = ckv_blk.shape[1]
        rope = kpe_blk.shape[2]
        scale = (w_uk.shape[1] + rope) ** -0.5
        me = lax.axis_index("sp")
        cos_t, sin_t = rope_tables(cache_len, rope)
        cos_t = jnp.concatenate([cos_t] * 4, axis=1)
        sin_t = jnp.concatenate([-sin_t, sin_t] * 2, axis=1)
        q_lat, q_pe, kv_new, c_new, k_new = project(hidden, cos_t, sin_t, w_dq, q_gain, w_uq, w_dkv.T, kv_gain, w_uk)
        info = jnp.stack([me * shard_len, me // 2]).astype(jnp.int32)
        ckv_out, kpe_out, o_parts, lse = attend(cache_len, info, q_lat, q_pe, c_new, k_new, ckv_blk, jnp.swapaxes(kpe_blk, 1, 2), scale)
        out = combine(o_parts, lse, w_uv, w_out)
        return out, ckv_out, jnp.swapaxes(kpe_out, 1, 2), kv_new

    cache_spec = P("dp", "sp", None)
    return jax.shard_map(local_step, mesh=mesh, in_specs=(P("dp", None), cache_spec, cache_spec, P("dp"), P(), P(), P(), P(), P(), P(), P(), P()), out_specs=(P("dp", None), cache_spec, cache_spec, P("dp", None)), check_vma=False)
```

```python
import functools

import jax
import jax.numpy as jnp
from jax import lax
from jax.experimental import pallas as pl
from jax.experimental.pallas import tpu as pltpu
from jax.sharding import PartitionSpec as P

EPS = 1e-6
ROPE_THETA = 10000.0
NEG_FILL = -1e30
MESH = pl.DeviceIdType.MESH
NBUF = 12
AHEAD = 6
OBUF = 4
TILE_T = 512
CHUNK = 4


def rope_tables(cache_len, rope_dim):
    inv_freq = jnp.power(ROPE_THETA, -2.0 * jnp.arange(rope_dim // 2, dtype=jnp.float32) / rope_dim)
    rope_angle = cache_len.astype(jnp.float32)[:, None] * inv_freq[None, :]
    return jnp.cos(rope_angle), jnp.sin(rope_angle)


def project_kernel(n_seqs, hid_ref, qg_ref, kvg_ref, cos_ref, sin_ref, wdq_hbm, wdkv_hbm, wuq_hbm, wuk_hbm,
                   lat_hbm, pe_hbm, kv_ref, cnew_ref, knew_ref, dq_buf, dkv_buf, uq_buf, uk_buf, q_mine, q_other,
                   lat_scr, pe_scr, lat_out, pe_out, dq_sem, dkv_sem, uq_sem, uk_sem, lo_sem, po_sem, q_s, q_r):
    core = lax.rem(lax.axis_index("sp"), 2)
    partner = lax.axis_index("sp") + 1 - 2 * core
    f32, bf16 = jnp.float32, jnp.bfloat16
    n_dq, rows, q_lora = dq_buf.shape
    tile = uq_buf.shape[2]
    n_tiles = q_mine.shape[0]
    lat = lat_scr.shape[2]
    uq_slots = uq_buf.shape[0]
    uk_slots = uk_buf.shape[0]

    def uq_copy(i):
        slot = lax.rem(i, uq_slots)
        col = pl.multiple_of(core * (n_tiles * tile) + i * tile, tile)
        return pltpu.make_async_copy(wuq_hbm.at[:, pl.ds(col, tile)], uq_buf.at[slot], uq_sem.at[slot])

    def uk_copy(i):
        half = i // 4
        head = (core + half - 2 * core * half) * 64 + lax.rem(i, 4) * 16
        slot = lax.rem(i, uk_slots)
        return pltpu.make_async_copy(wuk_hbm.at[pl.ds(head, 16)], uk_buf.at[slot], uk_sem.at[slot])

    dq_copies = [pltpu.make_async_copy(wdq_hbm.at[pl.ds(i * rows, rows)], dq_buf.at[i], dq_sem.at[i]) for i in range(n_dq)]
    dkv_copy = pltpu.make_async_copy(wdkv_hbm, dkv_buf, dkv_sem)
    for copy in dq_copies:
        copy.start()
    for i in range(uq_slots):
        uq_copy(jnp.int32(i)).start()
    dkv_copy.start()

    barrier = pltpu.get_barrier_semaphore()
    pl.semaphore_signal(barrier, inc=1, device_id={"sp": partner}, device_id_type=MESH)
    pl.semaphore_wait(barrier, 1)

    def norm(v, gain):
        mean_sq = jnp.mean(v * v, axis=-1, keepdims=True)
        return v * lax.rsqrt(mean_sq + EPS) * gain.astype(f32)

    acc = jnp.zeros((n_seqs, q_lora), f32)
    for i in range(n_dq):
        dq_copies[i].wait()
        acc = acc + jnp.dot(hid_ref[:, i * rows:(i + 1) * rows], dq_buf[i], preferred_element_type=f32)
    c_q = norm(acc, qg_ref[...]).astype(bf16)

    def q_send(i):
        return pltpu.make_async_remote_copy(src_ref=q_mine.at[i], dst_ref=q_other.at[i], send_sem=q_s.at[i], recv_sem=q_r.at[i],
                                            device_id={"sp": partner}, device_id_type=MESH)

    def q_tile(i, _):
        uq_copy(i).wait()
        q = jnp.dot(c_q, uq_buf[lax.rem(i, uq_slots)], preferred_element_type=f32)
        q_mine[i] = q.astype(bf16).astype(f32)

        @pl.when(i + uq_slots < n_tiles)
        def _():
            uq_copy(i + uq_slots).start()

        @pl.when(i == n_tiles - uq_slots)
        def _():
            for k in range(uk_slots):
                uk_copy(jnp.int32(k)).start()

        @pl.when(i > 0)
        def _():
            q_send(i - 1).start()
        return 0

    lax.fori_loop(0, n_tiles, q_tile, 0)
    cos_t, sin_t = cos_ref[...], sin_ref[...]
    lane = lax.broadcasted_iota(jnp.int32, (n_seqs, 128), 1)
    low_half = lax.rem(lane, 64) < 32

    def rotate_pairs(x):
        swapped = jnp.where(low_half, pltpu.roll(x, 96, 1), pltpu.roll(x, 32, 1))
        return x * cos_t + swapped * sin_t

    dkv_copy.wait()
    kv = lax.dot_general(hid_ref[...], dkv_buf[...], (((1,), (1,)), ((), ())), preferred_element_type=f32)
    q_send(jnp.int32(n_tiles - 1)).start()
    c_kv = norm(kv[:, :lat], kvg_ref[...]).astype(bf16)
    k_raw = jnp.concatenate([kv[:, lat:], jnp.zeros((n_seqs, 64), f32)], axis=1)
    k_pe = rotate_pairs(k_raw).astype(bf16)
    kv_ref[:, :lat] = c_kv
    kv_ref[:, lat:] = k_pe[:, :64]
    cnew_ref[...] = c_kv.astype(f32)
    square = jnp.concatenate([k_pe.astype(f32), jnp.zeros((128 - n_seqs, 128), f32)], axis=0)
    knew_ref[...] = jnp.transpose(square)[:64, :]

    def out_copies(half, g):
        return (pltpu.make_async_copy(lat_out.at[half, g], lat_hbm.at[half, :, pl.ds(g * 16, 16)], lo_sem.at[half, g]),
                pltpu.make_async_copy(pe_out.at[half, g], pe_hbm.at[half, :, pl.ds(g * 16, 16)], po_sem.at[half, g]))

    for half in range(2):
        src = q_mine if half == 0 else q_other

        def group(g, _, half=half, src=src):
            i = half * 4 + g
            uk_copy(i).wait()
            slot = lax.rem(i, uk_slots)
            if half == 1:
                q_send(2 * g).wait_recv()
                q_send(2 * g + 1).wait_recv()
            for h in range(0, 16, 2):
                t, p = divmod(h // 2, 4)
                v = src[2 * g + t, :, p * 384:(p + 1) * 384]
                even = v[:, :128].astype(bf16)
                odd = pltpu.roll(v, 192, 1)[:, :128].astype(bf16)
                x = jnp.where(lane < 64, v[:, 128:256], v[:, 256:384])
                rot = rotate_pairs(x)
                pe_scr[:, h, :] = rot
                pe_scr[:, h + 1, :] = pltpu.roll(rot, 64, 1)
                lat_scr[:, h, :] = jnp.dot(even, uk_buf[slot, h], preferred_element_type=f32)
                lat_scr[:, h + 1, :] = jnp.dot(odd, uk_buf[slot, h + 1], preferred_element_type=f32)
            lat_out[half, g] = lat_scr[...].astype(bf16)
            pe_out[half, g] = pe_scr[...][:, :, :64].astype(bf16)

            @pl.when(i + uk_slots < 8)
            def _():
                uk_copy(i + uk_slots).start()
            for copy in out_copies(half, g):
                copy.start()
            return 0

        lax.fori_loop(0, 4, group, 0)

    def drain(g, _):
        for half in range(2):
            for copy in out_copies(half, g):
                copy.wait()
        q_send(2 * g).wait_send()
        q_send(2 * g + 1).wait_send()
        return 0

    lax.fori_loop(0, 4, drain, 0)


def project(hidden, cos_t, sin_t, w_dq, q_gain, w_uq, w_dkv_t, kv_gain, w_uk):
    n_seqs, d_model = hidden.shape
    q_lora = w_dq.shape[1]
    n_heads, nope, lat = w_uk.shape
    rope = w_uq.shape[1] // n_heads - nope
    tile = 8 * (nope + rope)
    n_tiles = n_heads // 16
    n_dq, uq_slots, uk_slots = 8, 3, 4
    f32, bf16 = jnp.float32, jnp.bfloat16
    hbm = pl.BlockSpec(memory_space=pl.ANY)
    vmem = pl.BlockSpec(memory_space=pltpu.VMEM)
    dma = pltpu.SemaphoreType.DMA
    return pl.pallas_call(
        functools.partial(project_kernel, n_seqs),
        out_shape=[
            jax.ShapeDtypeStruct((2, n_seqs, 64, lat), bf16),
            jax.ShapeDtypeStruct((2, n_seqs, 64, rope), bf16),
            jax.ShapeDtypeStruct((n_seqs, lat + rope), bf16),
            jax.ShapeDtypeStruct((n_seqs, lat), f32),
            jax.ShapeDtypeStruct((rope, 128), f32),
        ],
        in_specs=[vmem] * 5 + [hbm] * 4,
        out_specs=[hbm, hbm, vmem, vmem, vmem],
        scratch_shapes=[
            pltpu.VMEM((n_dq, d_model // n_dq, q_lora), bf16),
            pltpu.VMEM((lat + rope, d_model), bf16),
            pltpu.VMEM((uq_slots, q_lora, tile), bf16),
            pltpu.VMEM((uk_slots, 16, nope, lat), bf16),
            pltpu.VMEM((n_tiles, n_seqs, tile), f32),
            pltpu.VMEM((n_tiles, n_seqs, tile), f32),
            pltpu.VMEM((n_seqs, 16, lat), f32),
            pltpu.VMEM((n_seqs, 16, 128), f32),
            pltpu.VMEM((2, 4, n_seqs, 16, lat), bf16),
            pltpu.VMEM((2, 4, n_seqs, 16, rope), bf16),
            dma((n_dq,)), dma, dma((uq_slots,)), dma((uk_slots,)), dma((2, 4)), dma((2, 4)), dma((n_tiles,)), dma((n_tiles,)),
        ],
        compiler_params=pltpu.CompilerParams(collective_id=1, has_side_effects=True, vmem_limit_bytes=60 * 1024 * 1024),
        name="project",
    )(hidden, q_gain[None, :], kv_gain[None, :], cos_t, sin_t, w_dq, w_dkv_t, w_uq, w_uk)


def attend_kernel(n_seqs, shard_len, scale, len_ref, cnew_ref, knew_ref, q_hbm, pe_hbm, ckv_hbm, kpe_hbm,
                  ckv_out, kpe_out, o_hbm, lse_ref, cbuf, kbuf, qbuf, pbuf, obuf, s_scr, lse_scr, in_sem, out_sem, o_sem):
    step = pl.program_id(0)
    me = lax.axis_index("sp")
    chip = me // 2

    def copies_in(seq):
        slot = lax.rem(seq, NBUF)
        return (pltpu.make_async_copy(q_hbm.at[:, seq], qbuf.at[slot], in_sem.at[2, slot]),
                pltpu.make_async_copy(pe_hbm.at[:, seq], pbuf.at[slot], in_sem.at[3, slot]),
                pltpu.make_async_copy(kpe_hbm.at[seq], kbuf.at[slot], in_sem.at[1, slot]),
                pltpu.make_async_copy(ckv_hbm.at[seq], cbuf.at[slot], in_sem.at[0, slot]))

    def copies_out(seq):
        slot = lax.rem(seq, NBUF)
        return (pltpu.make_async_copy(cbuf.at[slot], ckv_out.at[seq], out_sem.at[0, slot]),
                pltpu.make_async_copy(kbuf.at[slot], kpe_out.at[seq], out_sem.at[1, slot]))

    def copy_o(seq):
        slot = lax.rem(seq, OBUF)
        return pltpu.make_async_copy(obuf.at[slot], o_hbm.at[:, :, seq], o_sem.at[slot])

    @pl.when(step == 0)
    def _():
        for seq in range(AHEAD):
            for copy in copies_in(jnp.int32(seq)):
                copy.start()

    ahead = step + AHEAD

    @pl.when(ahead < n_seqs)
    def _():
        @pl.when(ahead >= NBUF)
        def _():
            for copy in copies_out(ahead - NBUF):
                copy.wait()
        for copy in copies_in(ahead):
            copy.start()

    for copy in copies_in(step):
        copy.wait()
    slot = lax.rem(step, NBUF)
    pos = len_ref[step] - me * shard_len

    @pl.when((pos >= 0) & (pos < shard_len))
    def _():
        row0 = pl.multiple_of((pos // 16) * 16, 16)
        block = cbuf[slot, pl.ds(row0, 16), :].astype(jnp.float32)
        rows = lax.broadcasted_iota(jnp.int32, block.shape, 0) + row0
        cbuf[slot, pl.ds(row0, 16), :] = jnp.where(rows == pos, cnew_ref[pl.ds(step, 1), :], block).astype(jnp.bfloat16)
        col0 = pl.multiple_of((pos // 128) * 128, 128)
        seq_lane = lax.broadcasted_iota(jnp.int32, knew_ref.shape, 1) == step
        new_col = jnp.sum(jnp.where(seq_lane, knew_ref[...], 0.0), axis=1, keepdims=True)
        kblock = kbuf[slot, :, pl.ds(col0, 128)].astype(jnp.float32)
        cols = lax.broadcasted_iota(jnp.int32, kblock.shape, 1) + col0
        kbuf[slot, :, pl.ds(col0, 128)] = jnp.where(cols == pos, new_col, kblock).astype(jnp.bfloat16)

    q_lat = jnp.concatenate([qbuf[slot, 0], qbuf[slot, 1]], axis=0)
    q_pe = jnp.concatenate([pbuf[slot, 0], pbuf[slot, 1]], axis=0)
    peak = None
    for t0 in range(0, shard_len, TILE_T):
        s = lax.dot_general(q_lat, cbuf[slot, t0:t0 + TILE_T, :], (((1,), (1,)), ((), ())), preferred_element_type=jnp.float32)
        s = s + lax.dot_general(q_pe, kbuf[slot, :, t0:t0 + TILE_T], (((1,), (0,)), ((), ())), preferred_element_type=jnp.float32)
        cols = lax.broadcasted_iota(jnp.int32, s.shape, 1) + t0
        s = jnp.where(cols <= pos, s * scale, NEG_FILL)
        s_scr[:, t0:t0 + TILE_T] = s
        tile_peak = jnp.max(s, axis=1, keepdims=True)
        peak = tile_peak if peak is None else jnp.maximum(peak, tile_peak)
    denom = jnp.zeros_like(peak)
    acc = None
    for t0 in range(0, shard_len, TILE_T):
        w = jnp.exp(s_scr[:, t0:t0 + TILE_T] - peak)
        denom = denom + jnp.sum(w, axis=1, keepdims=True)
        part = jnp.dot(w.astype(jnp.bfloat16), cbuf[slot, t0:t0 + TILE_T, :], preferred_element_type=jnp.float32)
        acc = part if acc is None else acc + part
    for copy in copies_out(step):
        copy.start()
    o = acc * (1.0 / denom)
    oslot = lax.rem(step, OBUF)

    @pl.when(step >= OBUF)
    def _():
        copy_o(step - OBUF).wait()
    for half in range(2):
        for group in range(4):
            r0 = half * 64 + group * 16
            obuf[oslot, half, group ^ chip] = o[r0:r0 + 16, :]
    copy_o(step).start()
    lanes = lax.broadcasted_iota(jnp.int32, lse_scr.shape, 1)
    lse_scr[...] = jnp.where(lanes == step, peak + jnp.log(denom), lse_scr[...])

    @pl.when(step == n_seqs - 1)
    def _():
        lse_ref[...] = jnp.transpose(lse_scr[...])[:n_seqs, :]
        for seq in range(n_seqs - NBUF, n_seqs):
            for copy in copies_out(jnp.int32(seq)):
                copy.wait()
        for seq in range(n_seqs - OBUF, n_seqs):
            copy_o(jnp.int32(seq)).wait()


def attend(cache_len, q_lat, q_pe, c_new, k_new, ckv, kpe_t, scale):
    n_seqs, shard_len, lat = ckv.shape
    rope = kpe_t.shape[1]
    whole = lambda shape: pl.BlockSpec(shape, lambda i, *_: (0,) * len(shape))
    hbm = pl.BlockSpec(memory_space=pl.ANY)
    return pl.pallas_call(
        functools.partial(attend_kernel, n_seqs, shard_len, scale),
        grid_spec=pltpu.PrefetchScalarGridSpec(
            num_scalar_prefetch=1,
            grid=(n_seqs,),
            in_specs=[whole((n_seqs, lat)), whole((rope, 128)), hbm, hbm, hbm, hbm],
            out_specs=[hbm, hbm, hbm, whole((n_seqs, 128))],
            scratch_shapes=[
                pltpu.VMEM((NBUF, shard_len, lat), jnp.bfloat16),
                pltpu.VMEM((NBUF, rope, shard_len), jnp.bfloat16),
                pltpu.VMEM((NBUF, 2, 64, lat), jnp.bfloat16),
                pltpu.VMEM((NBUF, 2, 64, rope), jnp.bfloat16),
                pltpu.VMEM((OBUF, 2, 4, 16, lat), jnp.float32),
                pltpu.VMEM((128, shard_len), jnp.float32),
                pltpu.VMEM((128, 128), jnp.float32),
                pltpu.SemaphoreType.DMA((4, NBUF)),
                pltpu.SemaphoreType.DMA((2, NBUF)),
                pltpu.SemaphoreType.DMA((OBUF,)),
            ],
        ),
        out_shape=[
            jax.ShapeDtypeStruct(ckv.shape, ckv.dtype),
            jax.ShapeDtypeStruct(kpe_t.shape, kpe_t.dtype),
            jax.ShapeDtypeStruct((2, 4, n_seqs, 16, lat), jnp.float32),
            jax.ShapeDtypeStruct((n_seqs, 128), jnp.float32),
        ],
        compiler_params=pltpu.CompilerParams(dimension_semantics=("arbitrary",), vmem_limit_bytes=60 * 1024 * 1024),
        name="attend",
    )(cache_len, c_new, k_new, q_lat, q_pe, ckv, kpe_t)


def combine_kernel(n_seqs, o_hbm, lse_ref, wuv_hbm, wout_hbm, out_ref, mine, got1, got2, got3, lse_all, w_mine, w_part,
                   wuv, wout, heads, part, part_got, quad, full, load_sem, wt_sem, d1_s, d1_r, s2_s, s2_r, s3_s, s3_r,
                   l_s, l_r, a_s, a_r, b_s, b_r, c_s, c_r, e_s, e_r):
    me = lax.axis_index("sp")
    core = lax.rem(me, 2)
    x_bit = lax.rem(me // 2, 2)
    y_bit = me // 4
    chip = me // 2

    def flip(bits):
        dev = me
        if bits & 1:
            dev = dev + 1 - 2 * core
        if bits & 2:
            dev = dev + 2 - 4 * x_bit
        if bits & 4:
            dev = dev + 4 - 8 * y_bit
        return dev

    def flip_chip(j):
        return (y_bit + (1 - 2 * y_bit if j & 2 else 0)) * 2 + x_bit + (1 - 2 * x_bit if j & 1 else 0)

    def send(src, dst, ssem, rsem, bits):
        return pltpu.make_async_remote_copy(src_ref=src, dst_ref=dst, send_sem=ssem, recv_sem=rsem,
                                            device_id={"sp": flip(bits)}, device_id_type=MESH)

    head0 = core * 64 + chip * 16
    wuv_copy = pltpu.make_async_copy(wuv_hbm.at[pl.ds(head0, 16)], wuv, wt_sem.at[0])
    wout_copy = pltpu.make_async_copy(wout_hbm.at[pl.ds(pl.multiple_of(head0 * 128, 2048), 2048)], wout, wt_sem.at[1])
    n_chunks = n_seqs // CHUNK
    loads = []
    for c in range(n_chunks):
        seqs = pl.ds(c * CHUNK, CHUNK)
        loads.append(pltpu.make_async_copy(o_hbm.at[0, :, seqs], mine.at[:, seqs], load_sem.at[c]))
        loads[c].start()
    wuv_copy.start()
    wout_copy.start()

    barrier = pltpu.get_barrier_semaphore()
    for bits in range(1, 8):
        pl.semaphore_signal(barrier, inc=1, device_id={"sp": flip(bits)}, device_id_type=MESH)
    pl.semaphore_wait(barrier, 7)

    lse_sends = [send(lse_ref, lse_all.at[bits], l_s.at[bits], l_r.at[bits], bits) for bits in range(1, 8)]
    for copy in lse_sends:
        copy.start()
    d1 = []
    for c in range(n_chunks):
        seqs = pl.ds(c * CHUNK, CHUNK)
        d1.append(send(o_hbm.at[1, :, seqs], got1.at[:, seqs], d1_s.at[c], d1_r.at[c], 1))
        d1[c].start()

    for copy in lse_sends:
        copy.wait_recv()
    lses = [lse_ref[...]]
    for bits in range(1, 8):
        other = lse_all[bits]
        lses.append(pltpu.roll(other, 64, 1) if bits & 1 else other)
    peak = functools.reduce(jnp.maximum, lses)
    total = functools.reduce(jnp.add, [jnp.exp(v - peak) for v in lses])
    norm = peak + jnp.log(total)
    pad = jnp.zeros((128 - n_seqs, 128), jnp.float32)
    for value, dst in ((lses[0], w_mine), (lses[1], w_part)):
        wt = jnp.transpose(jnp.concatenate([jnp.exp(value - norm), pad], axis=0))[:64, :]
        for s in range(n_seqs):
            dst[s] = jnp.broadcast_to(wt[:, s:s + 1], (64, 128))

    def orders(c):
        return (1, 2) if c % 2 == 0 else (2, 1)

    s2 = []
    for c in range(n_chunks):
        loads[c].wait()
        d1[c].wait_recv()
        for j in range(4):
            row0 = pl.multiple_of(flip_chip(j) * 16, 16)

            def merge(i, _, j=j, row0=row0, c=c):
                s = c * CHUNK + i
                wa = w_mine[s, pl.ds(row0, 16), :]
                wb = w_part[s, pl.ds(row0, 16), :]
                wa = jnp.concatenate([wa] * 4, axis=1)
                wb = jnp.concatenate([wb] * 4, axis=1)
                mine[j, s] = mine[j, s] * wa + got1[j, s] * wb
                return 0

            lax.fori_loop(0, CHUNK, merge, 0)
        first, _ = orders(c)
        seqs = pl.ds(c * CHUNK, CHUNK)
        s2.append((send(mine.at[first, seqs], got2.at[0, seqs], s2_s.at[0, c], s2_r.at[0, c], 2 * first),
                   send(mine.at[3, seqs], got2.at[1, seqs], s2_s.at[1, c], s2_r.at[1, c], 2 * first)))
        for copy in s2[c]:
            copy.start()

    s3 = []
    for c in range(n_chunks):
        _, second = orders(c)
        s2[c][0].wait_recv()
        s2[c][1].wait_recv()

        def add2(i, _, second=second, c=c):
            s = c * CHUNK + i
            mine[second, s] = mine[second, s] + got2[1, s]
            mine[0, s] = mine[0, s] + got2[0, s]
            return 0

        lax.fori_loop(0, CHUNK, add2, 0)
        seqs = pl.ds(c * CHUNK, CHUNK)
        s3.append(send(mine.at[second, seqs], got3.at[seqs], s3_s.at[c], s3_r.at[c], 2 * second))
        s3[c].start()

    for c in range(n_chunks):
        s3[c].wait_recv()

        def add3(i, _, c=c):
            s = c * CHUNK + i
            mine[0, s] = mine[0, s] + got3[s]
            return 0

        lax.fori_loop(0, CHUNK, add3, 0)

    wuv_copy.wait()
    for h in range(16):
        x = mine[0, :, h, :].astype(jnp.bfloat16)
        o = lax.dot_general(x, wuv[h], (((1,), (1,)), ((), ())), preferred_element_type=jnp.float32)
        heads[:, h * 128:(h + 1) * 128] = o.astype(jnp.bfloat16)
    wout_copy.wait()
    width = wout.shape[1] // 8

    def project_block(which, order):
        idx = flip_chip(order)
        col = pl.multiple_of((which * 4 + idx) * width, 128)
        part[which, idx] = jnp.dot(heads[...], wout[:, pl.ds(col, width)], preferred_element_type=jnp.float32)

    a = []
    for j in (3, 1, 2, 0):
        project_block(1 - core, j)
        idx = flip_chip(j)
        a.append(send(part.at[1 - core, idx], part_got.at[j], a_s.at[j], a_r.at[j], 1))
        a[-1].start()
    b = []
    for n, j in enumerate((3, 1, 2, 0)):
        project_block(core, j)
        idx = flip_chip(j)
        a[n].wait_recv()
        part[core, idx] = part[core, idx] + part_got[j]
        if j:
            b.append(send(part.at[core, idx], quad.at[j - 1], b_s.at[j - 1], b_r.at[j - 1], 2 * j))
            b[-1].start()
    for copy in b:
        copy.wait_recv()
    done = part[core, chip] + quad[0] + quad[1] + quad[2]
    full[core, chip] = done.astype(jnp.bfloat16).astype(jnp.float32)
    g = [send(full.at[core, chip], full.at[core, chip], c_s.at[j - 1], c_r.at[j - 1], 2 * j) for j in range(1, 4)]
    for copy in g:
        copy.start()
    e = []
    for n, j in enumerate((0, 2, 1, 3)):
        if j:
            g[j - 1].wait_recv()
        idx = flip_chip(j)
        e.append(send(full.at[core, idx], full.at[core, idx], e_s.at[j], e_r.at[j], 1))
        e[-1].start()
    for copy in e:
        copy.wait_recv()
    for p in range(8):
        out_ref[:, p * width:(p + 1) * width] = full[p // 4, p % 4].astype(jnp.bfloat16)

    for copy in lse_sends + d1 + [c for pair in s2 for c in pair] + s3 + a + b + g + e:
        copy.wait_send()


def combine(o_parts, lse, w_uv, w_out):
    _, _, n_seqs, _, lat = o_parts.shape
    d_model = w_out.shape[1]
    vdim = w_uv.shape[1]
    n_chunks = n_seqs // CHUNK
    width = d_model // 8
    hbm = pl.BlockSpec(memory_space=pl.ANY)
    vmem = pl.BlockSpec(memory_space=pltpu.VMEM)
    dma = pltpu.SemaphoreType.DMA
    f32 = jnp.float32
    return pl.pallas_call(
        functools.partial(combine_kernel, n_seqs),
        out_shape=jax.ShapeDtypeStruct((n_seqs, d_model), jnp.bfloat16),
        in_specs=[hbm, vmem, hbm, hbm],
        out_specs=vmem,
        scratch_shapes=[
            pltpu.VMEM((4, n_seqs, 16, lat), f32),
            pltpu.VMEM((4, n_seqs, 16, lat), f32),
            pltpu.VMEM((2, n_seqs, 16, lat), f32),
            pltpu.VMEM((n_seqs, 16, lat), f32),
            pltpu.VMEM((8, n_seqs, 128), f32),
            pltpu.VMEM((n_seqs, 64, 128), f32),
            pltpu.VMEM((n_seqs, 64, 128), f32),
            pltpu.VMEM((16, vdim, lat), jnp.bfloat16),
            pltpu.VMEM((16 * vdim, d_model), jnp.bfloat16),
            pltpu.VMEM((n_seqs, 16 * vdim), jnp.bfloat16),
            pltpu.VMEM((2, 4, n_seqs, width), f32),
            pltpu.VMEM((4, n_seqs, width), f32),
            pltpu.VMEM((3, n_seqs, width), f32),
            pltpu.VMEM((2, 4, n_seqs, width), f32),
            dma((n_chunks,)), dma((2,)),
            dma((n_chunks,)), dma((n_chunks,)),
            dma((2, n_chunks)), dma((2, n_chunks)),
            dma((n_chunks,)), dma((n_chunks,)),
            dma((8,)), dma((8,)),
            dma((4,)), dma((4,)), dma((3,)), dma((3,)), dma((3,)), dma((3,)), dma((4,)), dma((4,)),
        ],
        compiler_params=pltpu.CompilerParams(collective_id=0, has_side_effects=True, vmem_limit_bytes=60 * 1024 * 1024),
        name="combine",
    )(o_parts, lse, w_uv, w_out)


def solution(mesh):
    def local_step(hidden, ckv_blk, kpe_blk, cache_len, w_dq, q_gain, w_uq, w_dkv, kv_gain, w_uk, w_uv, w_out):
        rope = kpe_blk.shape[2]
        scale = (w_uk.shape[1] + rope) ** -0.5
        cos_t, sin_t = rope_tables(cache_len, rope)
        cos_t = jnp.concatenate([cos_t] * 4, axis=1)
        sin_t = jnp.concatenate([-sin_t, sin_t] * 2, axis=1)
        q_lat, q_pe, kv_new, c_new, k_new = project(hidden, cos_t, sin_t, w_dq, q_gain, w_uq, w_dkv.T, kv_gain, w_uk)
        ckv_out, kpe_out, o_parts, lse = attend(cache_len, q_lat, q_pe, c_new, k_new, ckv_blk, jnp.swapaxes(kpe_blk, 1, 2), scale)
        out = combine(o_parts, lse, w_uv, w_out)
        return out, ckv_out, jnp.swapaxes(kpe_out, 1, 2), kv_new

    cache_spec = P("dp", "sp", None)
    return jax.shard_map(local_step, mesh=mesh, in_specs=(P("dp", None), cache_spec, cache_spec, P("dp"), P(), P(), P(), P(), P(), P(), P(), P()), out_specs=(P("dp", None), cache_spec, cache_spec, P("dp", None)), check_vma=False)
```

```python
import functools

import jax
import jax.numpy as jnp
from jax import lax
from jax.experimental import pallas as pl
from jax.experimental.pallas import tpu as pltpu
from jax.sharding import PartitionSpec as P

EPS = 1e-6
ROPE_THETA = 10000.0
NEG_FILL = -1e30
MESH = pl.DeviceIdType.MESH
NBUF = 12
AHEAD = 6
OBUF = 4
TILE_T = 512
CHUNK = 8


def rope_tables(cache_len, rope_dim):
    inv_freq = jnp.power(ROPE_THETA, -2.0 * jnp.arange(rope_dim // 2, dtype=jnp.float32) / rope_dim)
    rope_angle = cache_len.astype(jnp.float32)[:, None] * inv_freq[None, :]
    return jnp.cos(rope_angle), jnp.sin(rope_angle)


def project_kernel(n_seqs, hid_ref, qg_ref, kvg_ref, cos_ref, sin_ref, wdq_hbm, wdkv_hbm, wuq_hbm, wuk_hbm,
                   lat_hbm, pe_hbm, kv_ref, cnew_ref, knew_ref, dq_buf, dkv_buf, uq_buf, uk_buf, cq_part, cq_got,
                   kv_part, kv_got, q_scr, lat_buf, lat_got, pe_buf, pe_got, lat_out, pe_out,
                   dq_sem, dkv_sem, uq_sem, uk_sem, lo_sem, po_sem, c_s, c_r, l_s, l_r, p_s, p_r):
    core = lax.rem(lax.axis_index("sp"), 2)
    partner = lax.axis_index("sp") + 1 - 2 * core
    f32, bf16 = jnp.float32, jnp.bfloat16
    n_dq, rows, q_lora = dq_buf.shape
    tile = uq_buf.shape[2]
    n_groups, _, _, lat = lat_buf.shape
    n_tiles = 2 * n_groups
    uq_slots = uq_buf.shape[0]
    k_half = n_dq * rows
    k0 = pl.multiple_of(core * k_half, 128)

    def uq_copy(i):
        slot = lax.rem(i, uq_slots)
        col = pl.multiple_of(core * (n_tiles * tile) + i * tile, tile)
        return pltpu.make_async_copy(wuq_hbm.at[:, pl.ds(col, tile)], uq_buf.at[slot], uq_sem.at[slot])

    def uk_copy(g):
        return pltpu.make_async_copy(wuk_hbm.at[pl.ds(core * 64 + g * 16, 16)], uk_buf.at[g], uk_sem.at[g])

    def swap(src, dst, ssem, rsem):
        return pltpu.make_async_remote_copy(src_ref=src, dst_ref=dst, send_sem=ssem, recv_sem=rsem,
                                            device_id={"sp": partner}, device_id_type=MESH)

    dq_copies = [pltpu.make_async_copy(wdq_hbm.at[pl.ds(pl.multiple_of(k0 + i * rows, 128), rows)], dq_buf.at[i], dq_sem.at[i])
                 for i in range(n_dq)]
    dkv_copy = pltpu.make_async_copy(wdkv_hbm.at[:, pl.ds(k0, k_half)], dkv_buf, dkv_sem)
    for copy in dq_copies:
        copy.start()
    dkv_copy.start()
    for g in range(2):
        uq_copy(jnp.int32(2 * g)).start()
        uq_copy(jnp.int32(2 * g + 1)).start()
        uk_copy(jnp.int32(g)).start()

    barrier = pltpu.get_barrier_semaphore()
    pl.semaphore_signal(barrier, inc=1, device_id={"sp": partner}, device_id_type=MESH)
    pl.semaphore_wait(barrier, 1)

    def norm(v, gain):
        mean_sq = jnp.mean(v * v, axis=-1, keepdims=True)
        return v * lax.rsqrt(mean_sq + EPS) * gain

    acc = jnp.zeros((n_seqs, q_lora), f32)
    for i in range(n_dq):
        dq_copies[i].wait()
        hid = hid_ref[:, pl.ds(pl.multiple_of(k0 + i * rows, 128), rows)]
        acc = acc + jnp.dot(hid, dq_buf[i], preferred_element_type=f32)
    cq_part[...] = acc
    cq_swap = swap(cq_part, cq_got, c_s.at[0], c_r.at[0])
    cq_swap.start()
    dkv_copy.wait()
    kv_part[...] = lax.dot_general(hid_ref[:, pl.ds(k0, k_half)], dkv_buf[...], (((1,), (1,)), ((), ())), preferred_element_type=f32)
    kv_swap = swap(kv_part, kv_got, c_s.at[1], c_r.at[1])
    kv_swap.start()
    cq_swap.wait_recv()
    c_q = norm(cq_part[...] + cq_got[...], qg_ref[...]).astype(bf16)

    cos_t, sin_t = cos_ref[...], sin_ref[...]
    lane = lax.broadcasted_iota(jnp.int32, (n_seqs, 128), 1)
    low_half = lax.rem(lane, 64) < 32

    def rotate_pairs(x):
        swapped = jnp.where(low_half, pltpu.roll(x, 96, 1), pltpu.roll(x, 32, 1))
        return x * cos_t + swapped * sin_t

    def out_copies(half, g):
        return (pltpu.make_async_copy(lat_out.at[half, g], lat_hbm.at[half, :, pl.ds(g * 16, 16)], lo_sem.at[half, g]),
                pltpu.make_async_copy(pe_out.at[half, g], pe_hbm.at[half, :, pl.ds(g * 16, 16)], po_sem.at[half, g]))

    def swaps(g):
        return (swap(lat_buf.at[g], lat_got.at[g], l_s.at[g], l_r.at[g]), swap(pe_buf.at[g], pe_got.at[g], p_s.at[g], p_r.at[g]))

    def group(g, _):
        for t in range(2):
            i = 2 * g + t
            uq_copy(i).wait()
            q = jnp.dot(c_q, uq_buf[lax.rem(i, uq_slots)], preferred_element_type=f32)
            q_scr[t] = q.astype(bf16).astype(f32)

            @pl.when(i + uq_slots < n_tiles)
            def _(i=i):
                uq_copy(i + uq_slots).start()

        @pl.when(g + 2 < n_groups)
        def _():
            uk_copy(g + 2).start()
        uk_copy(g).wait()
        for h in range(0, 16, 2):
            t, p = divmod(h // 2, 4)
            v = q_scr[t, :, p * 384:(p + 1) * 384]
            even = v[:, :128].astype(bf16)
            odd = pltpu.roll(v, 192, 1)[:, :128].astype(bf16)
            rot = rotate_pairs(jnp.where(lane < 64, v[:, 128:256], v[:, 256:384]))
            pe_buf[g, :, h, :] = rot
            pe_buf[g, :, h + 1, :] = pltpu.roll(rot, 64, 1)
            lat_buf[g, :, h, :] = jnp.dot(even, uk_buf[g, h], preferred_element_type=f32)
            lat_buf[g, :, h + 1, :] = jnp.dot(odd, uk_buf[g, h + 1], preferred_element_type=f32)
        lat_out[0, g] = lat_buf[g].astype(bf16)
        pe_out[0, g] = pe_buf[g][:, :, :64].astype(bf16)
        for copy in swaps(g):
            copy.start()
        for copy in out_copies(0, g):
            copy.start()
        return 0

    lax.fori_loop(0, n_groups, group, 0)

    kv_swap.wait_recv()
    kv = kv_part[...] + kv_got[...]
    c_kv = norm(kv[:, :lat], kvg_ref[...]).astype(bf16)
    k_raw = jnp.concatenate([kv[:, lat:], jnp.zeros((n_seqs, 64), f32)], axis=1)
    k_pe = rotate_pairs(k_raw).astype(bf16)
    kv_ref[:, :lat] = c_kv
    kv_ref[:, lat:] = k_pe[:, :64]
    cnew_ref[...] = c_kv.astype(f32)
    square = jnp.concatenate([k_pe.astype(f32), jnp.zeros((128 - n_seqs, 128), f32)], axis=0)
    knew_ref[...] = jnp.transpose(square)[:64, :]

    def receive(g, _):
        for copy in swaps(g):
            copy.wait_recv()
        lat_out[1, g] = lat_got[g].astype(bf16)
        pe_out[1, g] = pe_got[g][:, :, :64].astype(bf16)
        for copy in out_copies(1, g):
            copy.start()
        return 0

    lax.fori_loop(0, n_groups, receive, 0)

    def drain(g, _):
        for half in range(2):
            for copy in out_copies(half, g):
                copy.wait()
        for copy in swaps(g):
            copy.wait_send()
        return 0

    lax.fori_loop(0, n_groups, drain, 0)
    cq_swap.wait_send()
    kv_swap.wait_send()


def project(hidden, cos_t, sin_t, w_dq, q_gain, w_uq, w_dkv_t, kv_gain, w_uk):
    n_seqs, d_model = hidden.shape
    q_lora = w_dq.shape[1]
    n_heads, nope, lat = w_uk.shape
    rope = w_uq.shape[1] // n_heads - nope
    tile = 8 * (nope + rope)
    n_groups = n_heads // 32
    n_dq, uq_slots = 4, 4
    f32, bf16 = jnp.float32, jnp.bfloat16
    hbm = pl.BlockSpec(memory_space=pl.ANY)
    vmem = pl.BlockSpec(memory_space=pltpu.VMEM)
    dma = pltpu.SemaphoreType.DMA
    return pl.pallas_call(
        functools.partial(project_kernel, n_seqs),
        out_shape=[
            jax.ShapeDtypeStruct((2, n_seqs, 64, lat), bf16),
            jax.ShapeDtypeStruct((2, n_seqs, 64, rope), bf16),
            jax.ShapeDtypeStruct((n_seqs, lat + rope), bf16),
            jax.ShapeDtypeStruct((n_seqs, lat), f32),
            jax.ShapeDtypeStruct((rope, 128), f32),
        ],
        in_specs=[vmem] * 5 + [hbm] * 4,
        out_specs=[hbm, hbm, vmem, vmem, vmem],
        scratch_shapes=[
            pltpu.VMEM((n_dq, d_model // (2 * n_dq), q_lora), bf16),
            pltpu.VMEM((lat + rope, d_model // 2), bf16),
            pltpu.VMEM((uq_slots, q_lora, tile), bf16),
            pltpu.VMEM((n_groups, 16, nope, lat), bf16),
            pltpu.VMEM((n_seqs, q_lora), f32),
            pltpu.VMEM((n_seqs, q_lora), f32),
            pltpu.VMEM((n_seqs, lat + rope), f32),
            pltpu.VMEM((n_seqs, lat + rope), f32),
            pltpu.VMEM((2, n_seqs, tile), f32),
            pltpu.VMEM((n_groups, n_seqs, 16, lat), f32),
            pltpu.VMEM((n_groups, n_seqs, 16, lat), f32),
            pltpu.VMEM((n_groups, n_seqs, 16, 128), f32),
            pltpu.VMEM((n_groups, n_seqs, 16, 128), f32),
            pltpu.VMEM((2, n_groups, n_seqs, 16, lat), bf16),
            pltpu.VMEM((2, n_groups, n_seqs, 16, rope), bf16),
            dma((n_dq,)), dma, dma((uq_slots,)), dma((n_groups,)), dma((2, n_groups)), dma((2, n_groups)), dma((2,)), dma((2,)),
            dma((n_groups,)), dma((n_groups,)), dma((n_groups,)), dma((n_groups,)),
        ],
        compiler_params=pltpu.CompilerParams(collective_id=1, has_side_effects=True, vmem_limit_bytes=60 * 1024 * 1024),
        name="project",
    )(hidden, q_gain.astype(f32)[None, :], kv_gain.astype(f32)[None, :], cos_t, sin_t, w_dq, w_dkv_t, w_uq, w_uk)


def attend_kernel(n_seqs, shard_len, scale, len_ref, cnew_ref, knew_ref, q_hbm, pe_hbm, ckv_hbm, kpe_hbm,
                  ckv_out, kpe_out, o_hbm, lse_ref, cbuf, kbuf, qbuf, pbuf, obuf, s_scr, lse_scr, in_sem, out_sem, o_sem):
    step = pl.program_id(0)
    me = lax.axis_index("sp")
    chip = me // 2

    def copies_in(seq):
        slot = lax.rem(seq, NBUF)
        return (pltpu.make_async_copy(q_hbm.at[:, seq], qbuf.at[slot], in_sem.at[2, slot]),
                pltpu.make_async_copy(pe_hbm.at[:, seq], pbuf.at[slot], in_sem.at[3, slot]),
                pltpu.make_async_copy(kpe_hbm.at[seq], kbuf.at[slot], in_sem.at[1, slot]),
                pltpu.make_async_copy(ckv_hbm.at[seq], cbuf.at[slot], in_sem.at[0, slot]))

    def copies_out(seq):
        slot = lax.rem(seq, NBUF)
        return (pltpu.make_async_copy(cbuf.at[slot], ckv_out.at[seq], out_sem.at[0, slot]),
                pltpu.make_async_copy(kbuf.at[slot], kpe_out.at[seq], out_sem.at[1, slot]))

    def copy_o(seq):
        slot = lax.rem(seq, OBUF)
        return pltpu.make_async_copy(obuf.at[slot], o_hbm.at[:, :, seq], o_sem.at[slot])

    @pl.when(step == 0)
    def _():
        for seq in range(AHEAD):
            for copy in copies_in(jnp.int32(seq)):
                copy.start()

    ahead = step + AHEAD

    @pl.when(ahead < n_seqs)
    def _():
        @pl.when(ahead >= NBUF)
        def _():
            for copy in copies_out(ahead - NBUF):
                copy.wait()
        for copy in copies_in(ahead):
            copy.start()

    for copy in copies_in(step):
        copy.wait()
    slot = lax.rem(step, NBUF)
    pos = len_ref[step] - me * shard_len

    @pl.when((pos >= 0) & (pos < shard_len))
    def _():
        row0 = pl.multiple_of((pos // 16) * 16, 16)
        block = cbuf[slot, pl.ds(row0, 16), :].astype(jnp.float32)
        rows = lax.broadcasted_iota(jnp.int32, block.shape, 0) + row0
        cbuf[slot, pl.ds(row0, 16), :] = jnp.where(rows == pos, cnew_ref[pl.ds(step, 1), :], block).astype(jnp.bfloat16)
        col0 = pl.multiple_of((pos // 128) * 128, 128)
        seq_lane = lax.broadcasted_iota(jnp.int32, knew_ref.shape, 1) == step
        new_col = jnp.sum(jnp.where(seq_lane, knew_ref[...], 0.0), axis=1, keepdims=True)
        kblock = kbuf[slot, :, pl.ds(col0, 128)].astype(jnp.float32)
        cols = lax.broadcasted_iota(jnp.int32, kblock.shape, 1) + col0
        kbuf[slot, :, pl.ds(col0, 128)] = jnp.where(cols == pos, new_col, kblock).astype(jnp.bfloat16)

    q_lat = jnp.concatenate([qbuf[slot, 0], qbuf[slot, 1]], axis=0)
    q_pe = jnp.concatenate([pbuf[slot, 0], pbuf[slot, 1]], axis=0)
    peak = None
    for t0 in range(0, shard_len, TILE_T):
        s = lax.dot_general(q_lat, cbuf[slot, t0:t0 + TILE_T, :], (((1,), (1,)), ((), ())), preferred_element_type=jnp.float32)
        s = s + lax.dot_general(q_pe, kbuf[slot, :, t0:t0 + TILE_T], (((1,), (0,)), ((), ())), preferred_element_type=jnp.float32)
        cols = lax.broadcasted_iota(jnp.int32, s.shape, 1) + t0
        s = jnp.where(cols <= pos, s * scale, NEG_FILL)
        s_scr[:, t0:t0 + TILE_T] = s
        tile_peak = jnp.max(s, axis=1, keepdims=True)
        peak = tile_peak if peak is None else jnp.maximum(peak, tile_peak)
    denom = jnp.zeros_like(peak)
    acc = None
    for t0 in range(0, shard_len, TILE_T):
        w = jnp.exp(s_scr[:, t0:t0 + TILE_T] - peak)
        denom = denom + jnp.sum(w, axis=1, keepdims=True)
        part = jnp.dot(w.astype(jnp.bfloat16), cbuf[slot, t0:t0 + TILE_T, :], preferred_element_type=jnp.float32)
        acc = part if acc is None else acc + part
    for copy in copies_out(step):
        copy.start()
    o = acc * (1.0 / denom)
    oslot = lax.rem(step, OBUF)

    @pl.when(step >= OBUF)
    def _():
        copy_o(step - OBUF).wait()
    for half in range(2):
        for group in range(4):
            r0 = half * 64 + group * 16
            obuf[oslot, half, group ^ chip] = o[r0:r0 + 16, :]
    copy_o(step).start()
    lanes = lax.broadcasted_iota(jnp.int32, lse_scr.shape, 1)
    lse_scr[...] = jnp.where(lanes == step, peak + jnp.log(denom), lse_scr[...])

    @pl.when(step == n_seqs - 1)
    def _():
        lse_ref[...] = jnp.transpose(lse_scr[...])[:n_seqs, :]
        for seq in range(n_seqs - NBUF, n_seqs):
            for copy in copies_out(jnp.int32(seq)):
                copy.wait()
        for seq in range(n_seqs - OBUF, n_seqs):
            copy_o(jnp.int32(seq)).wait()


def attend(cache_len, q_lat, q_pe, c_new, k_new, ckv, kpe_t, scale):
    n_seqs, shard_len, lat = ckv.shape
    rope = kpe_t.shape[1]
    whole = lambda shape: pl.BlockSpec(shape, lambda i, *_: (0,) * len(shape))
    hbm = pl.BlockSpec(memory_space=pl.ANY)
    return pl.pallas_call(
        functools.partial(attend_kernel, n_seqs, shard_len, scale),
        grid_spec=pltpu.PrefetchScalarGridSpec(
            num_scalar_prefetch=1,
            grid=(n_seqs,),
            in_specs=[whole((n_seqs, lat)), whole((rope, 128)), hbm, hbm, hbm, hbm],
            out_specs=[hbm, hbm, hbm, whole((n_seqs, 128))],
            scratch_shapes=[
                pltpu.VMEM((NBUF, shard_len, lat), jnp.bfloat16),
                pltpu.VMEM((NBUF, rope, shard_len), jnp.bfloat16),
                pltpu.VMEM((NBUF, 2, 64, lat), jnp.bfloat16),
                pltpu.VMEM((NBUF, 2, 64, rope), jnp.bfloat16),
                pltpu.VMEM((OBUF, 2, 4, 16, lat), jnp.float32),
                pltpu.VMEM((128, shard_len), jnp.float32),
                pltpu.VMEM((128, 128), jnp.float32),
                pltpu.SemaphoreType.DMA((4, NBUF)),
                pltpu.SemaphoreType.DMA((2, NBUF)),
                pltpu.SemaphoreType.DMA((OBUF,)),
            ],
        ),
        out_shape=[
            jax.ShapeDtypeStruct(ckv.shape, ckv.dtype),
            jax.ShapeDtypeStruct(kpe_t.shape, kpe_t.dtype),
            jax.ShapeDtypeStruct((2, 4, n_seqs, 16, lat), jnp.float32),
            jax.ShapeDtypeStruct((n_seqs, 128), jnp.float32),
        ],
        compiler_params=pltpu.CompilerParams(dimension_semantics=("arbitrary",), vmem_limit_bytes=60 * 1024 * 1024),
        name="attend",
    )(cache_len, c_new, k_new, q_lat, q_pe, ckv, kpe_t)


def combine_kernel(n_seqs, o_hbm, lse_ref, wuv_hbm, wout_hbm, out_ref, mine, got1, got2, got3, lse_all, w_mine, w_part,
                   wuv, wout, heads, part, part_got, quad, full, load_sem, wt_sem, d1_s, d1_r, s2_s, s2_r, s3_s, s3_r,
                   l_s, l_r, a_s, a_r, b_s, b_r, c_s, c_r, e_s, e_r):
    me = lax.axis_index("sp")
    core = lax.rem(me, 2)
    x_bit = lax.rem(me // 2, 2)
    y_bit = me // 4
    chip = me // 2

    def flip(bits):
        dev = me
        if bits & 1:
            dev = dev + 1 - 2 * core
        if bits & 2:
            dev = dev + 2 - 4 * x_bit
        if bits & 4:
            dev = dev + 4 - 8 * y_bit
        return dev

    def flip_chip(j):
        return (y_bit + (1 - 2 * y_bit if j & 2 else 0)) * 2 + x_bit + (1 - 2 * x_bit if j & 1 else 0)

    def send(src, dst, ssem, rsem, bits):
        return pltpu.make_async_remote_copy(src_ref=src, dst_ref=dst, send_sem=ssem, recv_sem=rsem,
                                            device_id={"sp": flip(bits)}, device_id_type=MESH)

    head0 = core * 64 + chip * 16
    wuv_copy = pltpu.make_async_copy(wuv_hbm.at[pl.ds(head0, 16)], wuv, wt_sem.at[0])
    wout_copy = pltpu.make_async_copy(wout_hbm.at[pl.ds(pl.multiple_of(head0 * 128, 2048), 2048)], wout, wt_sem.at[1])
    per_half = n_seqs // CHUNK
    n_chunks = 2 * per_half

    def span(c):
        return pl.ds((c % per_half) * CHUNK, CHUNK), pl.ds((c // per_half) * 8, 8)

    loads = []
    for c in range(n_chunks):
        seqs, hs = span(c)
        loads.append(pltpu.make_async_copy(o_hbm.at[0, :, seqs, hs], mine.at[:, seqs, hs], load_sem.at[c]))
        loads[c].start()
    wuv_copy.start()
    wout_copy.start()

    barrier = pltpu.get_barrier_semaphore()
    for bits in range(1, 8):
        pl.semaphore_signal(barrier, inc=1, device_id={"sp": flip(bits)}, device_id_type=MESH)
    pl.semaphore_wait(barrier, 7)

    lse_sends = [send(lse_ref, lse_all.at[bits], l_s.at[bits], l_r.at[bits], bits) for bits in range(1, 8)]
    for copy in lse_sends:
        copy.start()
    d1 = []
    for c in range(n_chunks):
        seqs, hs = span(c)
        d1.append(send(o_hbm.at[1, :, seqs, hs], got1.at[:, seqs, hs], d1_s.at[c], d1_r.at[c], 1))
        d1[c].start()

    for copy in lse_sends:
        copy.wait_recv()
    lses = [lse_ref[...]]
    for bits in range(1, 8):
        other = lse_all[bits]
        lses.append(pltpu.roll(other, 64, 1) if bits & 1 else other)
    peak = functools.reduce(jnp.maximum, lses)
    total = functools.reduce(jnp.add, [jnp.exp(v - peak) for v in lses])
    norm = peak + jnp.log(total)
    pad = jnp.zeros((128 - n_seqs, 128), jnp.float32)
    for value, dst in ((lses[0], w_mine), (lses[1], w_part)):
        wt = jnp.transpose(jnp.concatenate([jnp.exp(value - norm), pad], axis=0))[:64, :]
        for s in range(n_seqs):
            dst[s] = jnp.broadcast_to(wt[:, s:s + 1], (64, 128))

    def orders(c):
        return (1, 2) if c % 2 == 0 else (2, 1)

    s2 = []
    for c in range(n_chunks):
        loads[c].wait()
        d1[c].wait_recv()
        seqs, hs = span(c)
        head = (c // per_half) * 8
        for j in range(4):
            row0 = pl.multiple_of(flip_chip(j) * 16 + head, 8)

            def merge(i, _, j=j, row0=row0, c=c, hs=hs):
                s = (c % per_half) * CHUNK + i
                wa = w_mine[s, pl.ds(row0, 8), :]
                wb = w_part[s, pl.ds(row0, 8), :]
                wa = jnp.concatenate([wa] * 4, axis=1)
                wb = jnp.concatenate([wb] * 4, axis=1)
                mine[j, s, hs] = mine[j, s, hs] * wa + got1[j, s, hs] * wb
                return 0

            lax.fori_loop(0, CHUNK, merge, 0, unroll=4)
        first, _ = orders(c)
        s2.append((send(mine.at[first, seqs, hs], got2.at[0, seqs, hs], s2_s.at[0, c], s2_r.at[0, c], 2 * first),
                   send(mine.at[3, seqs, hs], got2.at[1, seqs, hs], s2_s.at[1, c], s2_r.at[1, c], 2 * first)))
        for copy in s2[c]:
            copy.start()

    s3 = []
    for c in range(n_chunks):
        _, second = orders(c)
        s2[c][0].wait_recv()
        s2[c][1].wait_recv()
        seqs, hs = span(c)
        mine[second, seqs, hs] = mine[second, seqs, hs] + got2[1, seqs, hs]
        s3.append(send(mine.at[second, seqs, hs], got3.at[seqs, hs], s3_s.at[c], s3_r.at[c], 2 * second))
        mine[0, seqs, hs] = mine[0, seqs, hs] + got2[0, seqs, hs]
        s3[c].start()

    def latents(c):
        s3[c].wait_recv()
        seqs, hs = span(c)
        mine[0, seqs, hs] = mine[0, seqs, hs] + got3[seqs, hs]

    def value_heads(h0):
        for h in range(h0, h0 + 8):
            x = mine[0, :, h, :].astype(jnp.bfloat16)
            o = lax.dot_general(x, wuv[h], (((1,), (1,)), ((), ())), preferred_element_type=jnp.float32)
            heads[:, h * 128:(h + 1) * 128] = o.astype(jnp.bfloat16)

    width = wout.shape[1] // 8
    depth = wout.shape[0] // 2

    for c in range(per_half):
        latents(c)
    wuv_copy.wait()
    value_heads(0)
    wout_copy.wait()
    for p in range(8):
        part[p // 4, p % 4] = jnp.dot(heads[:, :depth], wout[:depth, p * width:(p + 1) * width], preferred_element_type=jnp.float32)
    for c in range(per_half, n_chunks):
        latents(c)
    value_heads(8)

    def project_block(which, order):
        idx = flip_chip(order)
        col = pl.multiple_of((which * 4 + idx) * width, 128)
        part[which, idx] = part[which, idx] + jnp.dot(heads[:, depth:], wout[depth:, pl.ds(col, width)], preferred_element_type=jnp.float32)

    a = []
    for j in (3, 1, 2, 0):
        project_block(1 - core, j)
        idx = flip_chip(j)
        a.append(send(part.at[1 - core, idx], part_got.at[j], a_s.at[j], a_r.at[j], 1))
        a[-1].start()
    b = []
    for n, j in enumerate((3, 1, 2, 0)):
        project_block(core, j)
        idx = flip_chip(j)
        a[n].wait_recv()
        part[core, idx] = part[core, idx] + part_got[j]
        if j:
            b.append(send(part.at[core, idx], quad.at[j - 1], b_s.at[j - 1], b_r.at[j - 1], 2 * j))
            b[-1].start()
    for copy in b:
        copy.wait_recv()
    done = part[core, chip] + quad[0] + quad[1] + quad[2]
    full[core, chip] = done.astype(jnp.bfloat16).astype(jnp.float32)
    g = [send(full.at[core, chip], full.at[core, chip], c_s.at[j - 1], c_r.at[j - 1], 2 * j) for j in range(1, 4)]
    for copy in g:
        copy.start()
    e = []
    for n, j in enumerate((0, 2, 1, 3)):
        if j:
            g[j - 1].wait_recv()
        idx = flip_chip(j)
        e.append(send(full.at[core, idx], full.at[core, idx], e_s.at[j], e_r.at[j], 1))
        e[-1].start()
    for copy in e:
        copy.wait_recv()
    for p in range(8):
        out_ref[:, p * width:(p + 1) * width] = full[p // 4, p % 4].astype(jnp.bfloat16)

    for copy in lse_sends + d1 + [c for pair in s2 for c in pair] + s3 + a + b + g + e:
        copy.wait_send()


def combine(o_parts, lse, w_uv, w_out):
    _, _, n_seqs, _, lat = o_parts.shape
    d_model = w_out.shape[1]
    vdim = w_uv.shape[1]
    n_chunks = 2 * n_seqs // CHUNK
    width = d_model // 8
    hbm = pl.BlockSpec(memory_space=pl.ANY)
    vmem = pl.BlockSpec(memory_space=pltpu.VMEM)
    dma = pltpu.SemaphoreType.DMA
    f32 = jnp.float32
    return pl.pallas_call(
        functools.partial(combine_kernel, n_seqs),
        out_shape=jax.ShapeDtypeStruct((n_seqs, d_model), jnp.bfloat16),
        in_specs=[hbm, vmem, hbm, hbm],
        out_specs=vmem,
        scratch_shapes=[
            pltpu.VMEM((4, n_seqs, 16, lat), f32),
            pltpu.VMEM((4, n_seqs, 16, lat), f32),
            pltpu.VMEM((2, n_seqs, 16, lat), f32),
            pltpu.VMEM((n_seqs, 16, lat), f32),
            pltpu.VMEM((8, n_seqs, 128), f32),
            pltpu.VMEM((n_seqs, 64, 128), f32),
            pltpu.VMEM((n_seqs, 64, 128), f32),
            pltpu.VMEM((16, vdim, lat), jnp.bfloat16),
            pltpu.VMEM((16 * vdim, d_model), jnp.bfloat16),
            pltpu.VMEM((n_seqs, 16 * vdim), jnp.bfloat16),
            pltpu.VMEM((2, 4, n_seqs, width), f32),
            pltpu.VMEM((4, n_seqs, width), f32),
            pltpu.VMEM((3, n_seqs, width), f32),
            pltpu.VMEM((2, 4, n_seqs, width), f32),
            dma((n_chunks,)), dma((2,)),
            dma((n_chunks,)), dma((n_chunks,)),
            dma((2, n_chunks)), dma((2, n_chunks)),
            dma((n_chunks,)), dma((n_chunks,)),
            dma((8,)), dma((8,)),
            dma((4,)), dma((4,)), dma((3,)), dma((3,)), dma((3,)), dma((3,)), dma((4,)), dma((4,)),
        ],
        compiler_params=pltpu.CompilerParams(collective_id=0, has_side_effects=True, vmem_limit_bytes=60 * 1024 * 1024),
        name="combine",
    )(o_parts, lse, w_uv, w_out)


def solution(mesh):
    def local_step(hidden, ckv_blk, kpe_blk, cache_len, w_dq, q_gain, w_uq, w_dkv, kv_gain, w_uk, w_uv, w_out):
        rope = kpe_blk.shape[2]
        scale = (w_uk.shape[1] + rope) ** -0.5
        cos_t, sin_t = rope_tables(cache_len, rope)
        cos_t = jnp.concatenate([cos_t] * 4, axis=1)
        sin_t = jnp.concatenate([-sin_t, sin_t] * 2, axis=1)
        q_lat, q_pe, kv_new, c_new, k_new = project(hidden, cos_t, sin_t, w_dq, q_gain, w_uq, w_dkv.T, kv_gain, w_uk)
        ckv_out, kpe_out, o_parts, lse = attend(cache_len, q_lat, q_pe, c_new, k_new, ckv_blk, jnp.swapaxes(kpe_blk, 1, 2), scale)
        out = combine(o_parts, lse, w_uv, w_out)
        return out, ckv_out, jnp.swapaxes(kpe_out, 1, 2), kv_new

    cache_spec = P("dp", "sp", None)
    return jax.shard_map(local_step, mesh=mesh, in_specs=(P("dp", None), cache_spec, cache_spec, P("dp"), P(), P(), P(), P(), P(), P(), P(), P()), out_specs=(P("dp", None), cache_spec, cache_spec, P("dp", None)), check_vma=False)
```

```python
import functools

import jax
import jax.numpy as jnp
from jax import lax
from jax.experimental import pallas as pl
from jax.experimental.pallas import tpu as pltpu
from jax.sharding import PartitionSpec as P

EPS = 1e-6
ROPE_THETA = 10000.0
NEG_FILL = -1e30
MESH = pl.DeviceIdType.MESH
NBUF = 12
AHEAD = 6
OBUF = 4
TILE_T = 512
CHUNK = 8


def rope_tables(cache_len, rope_dim):
    inv_freq = jnp.power(ROPE_THETA, -2.0 * jnp.arange(rope_dim // 2, dtype=jnp.float32) / rope_dim)
    rope_angle = cache_len.astype(jnp.float32)[:, None] * inv_freq[None, :]
    return jnp.cos(rope_angle), jnp.sin(rope_angle)


def project_kernel(n_seqs, hid_ref, qg_ref, kvg_ref, cos_ref, sin_ref, wdq_hbm, wdkv_hbm, wuq_hbm, wuk_hbm,
                   lat_hbm, pe_hbm, kv_ref, cnew_ref, knew_ref, dq_buf, dkv_buf, uq_buf, uk_buf, cq_part, cq_got,
                   kv_part, kv_got, q_scr, lat_buf, lat_got, pe_buf, pe_got, lat_out, pe_out,
                   dq_sem, dkv_sem, uq_sem, uk_sem, lo_sem, po_sem, c_s, c_r, l_s, l_r, p_s, p_r):
    core = lax.rem(lax.axis_index("sp"), 2)
    partner = lax.axis_index("sp") + 1 - 2 * core
    f32, bf16 = jnp.float32, jnp.bfloat16
    n_dq, rows, q_lora = dq_buf.shape
    tile = uq_buf.shape[2]
    n_groups, _, _, lat = lat_buf.shape
    n_tiles = 2 * n_groups
    uq_slots = uq_buf.shape[0]
    k_half = n_dq * rows
    k0 = pl.multiple_of(core * k_half, 128)

    def uq_copy(i):
        slot = lax.rem(i, uq_slots)
        col = pl.multiple_of(core * (n_tiles * tile) + i * tile, tile)
        return pltpu.make_async_copy(wuq_hbm.at[:, pl.ds(col, tile)], uq_buf.at[slot], uq_sem.at[slot])

    def uk_copy(g):
        return pltpu.make_async_copy(wuk_hbm.at[pl.ds(core * 64 + g * 16, 16)], uk_buf.at[g], uk_sem.at[g])

    def swap(src, dst, ssem, rsem):
        return pltpu.make_async_remote_copy(src_ref=src, dst_ref=dst, send_sem=ssem, recv_sem=rsem,
                                            device_id={"sp": partner}, device_id_type=MESH)

    dq_copies = [pltpu.make_async_copy(wdq_hbm.at[pl.ds(pl.multiple_of(k0 + i * rows, 128), rows)], dq_buf.at[i], dq_sem.at[i])
                 for i in range(n_dq)]
    dkv_copy = pltpu.make_async_copy(wdkv_hbm.at[:, pl.ds(k0, k_half)], dkv_buf, dkv_sem)
    for copy in dq_copies:
        copy.start()
    dkv_copy.start()
    for g in range(2):
        uq_copy(jnp.int32(2 * g)).start()
        uq_copy(jnp.int32(2 * g + 1)).start()
        uk_copy(jnp.int32(g)).start()

    barrier = pltpu.get_barrier_semaphore()
    pl.semaphore_signal(barrier, inc=1, device_id={"sp": partner}, device_id_type=MESH)
    pl.semaphore_wait(barrier, 1)

    def norm(v, gain):
        mean_sq = jnp.mean(v * v, axis=-1, keepdims=True)
        return v * lax.rsqrt(mean_sq + EPS) * gain.astype(f32)[None, :]

    acc = jnp.zeros((n_seqs, q_lora), f32)
    for i in range(n_dq):
        dq_copies[i].wait()
        hid = hid_ref[:, pl.ds(pl.multiple_of(k0 + i * rows, 128), rows)]
        acc = acc + jnp.dot(hid, dq_buf[i], preferred_element_type=f32)
    cq_part[...] = acc
    cq_swap = swap(cq_part, cq_got, c_s.at[0], c_r.at[0])
    cq_swap.start()
    dkv_copy.wait()
    kv_part[...] = lax.dot_general(hid_ref[:, pl.ds(k0, k_half)], dkv_buf[...], (((1,), (1,)), ((), ())), preferred_element_type=f32)
    kv_swap = swap(kv_part, kv_got, c_s.at[1], c_r.at[1])
    kv_swap.start()
    cq_swap.wait_recv()
    c_q = norm(cq_part[...] + cq_got[...], qg_ref[...]).astype(bf16)

    cos_t, sin_t = cos_ref[...], sin_ref[...]
    lane = lax.broadcasted_iota(jnp.int32, (n_seqs, 128), 1)
    low_half = lax.rem(lane, 64) < 32

    def rotate_pairs(x):
        swapped = jnp.where(low_half, pltpu.roll(x, 96, 1), pltpu.roll(x, 32, 1))
        return x * cos_t + swapped * sin_t

    def out_copies(half, g):
        return (pltpu.make_async_copy(lat_out.at[half, g], lat_hbm.at[half, :, pl.ds(g * 16, 16)], lo_sem.at[half, g]),
                pltpu.make_async_copy(pe_out.at[half, g], pe_hbm.at[half, :, pl.ds(g * 16, 16)], po_sem.at[half, g]))

    def swaps(g):
        return (swap(lat_buf.at[g], lat_got.at[g], l_s.at[g], l_r.at[g]), swap(pe_buf.at[g], pe_got.at[g], p_s.at[g], p_r.at[g]))

    kv_swap.wait_recv()
    kv = kv_part[...] + kv_got[...]
    c_kv = norm(kv[:, :lat], kvg_ref[...]).astype(bf16)
    k_raw = jnp.concatenate([kv[:, lat:], jnp.zeros((n_seqs, 64), f32)], axis=1)
    k_pe = rotate_pairs(k_raw).astype(bf16)
    kv_ref[:, :lat] = c_kv
    kv_ref[:, lat:] = k_pe[:, :64]
    cnew_ref[...] = c_kv.astype(f32)
    square = jnp.concatenate([k_pe.astype(f32), jnp.zeros((128 - n_seqs, 128), f32)], axis=0)
    knew_ref[...] = jnp.transpose(square)[:64, :]

    def receive(g):
        for copy in swaps(g):
            copy.wait_recv()
        lat_out[1, g] = lat_got[g].astype(bf16)
        pe_out[1, g] = pe_got[g][:, :, :64].astype(bf16)
        for copy in out_copies(1, g):
            copy.start()

    def group(g, _):
        for t in range(2):
            i = 2 * g + t
            uq_copy(i).wait()
            q = jnp.dot(c_q, uq_buf[lax.rem(i, uq_slots)], preferred_element_type=f32)
            q_scr[t] = q.astype(bf16).astype(f32)

            @pl.when(i + uq_slots < n_tiles)
            def _(i=i):
                uq_copy(i + uq_slots).start()

        @pl.when(g + 2 < n_groups)
        def _():
            uk_copy(g + 2).start()
        uk_copy(g).wait()
        for h in range(0, 16, 2):
            t, p = divmod(h // 2, 4)
            v = q_scr[t, :, p * 384:(p + 1) * 384]
            even = v[:, :128].astype(bf16)
            odd = pltpu.roll(v, 192, 1)[:, :128].astype(bf16)
            rot = rotate_pairs(jnp.where(lane < 64, v[:, 128:256], v[:, 256:384]))
            pe_buf[g, :, h, :] = rot
            pe_buf[g, :, h + 1, :] = pltpu.roll(rot, 64, 1)
            lat_buf[g, :, h, :] = jnp.dot(even, uk_buf[g, h], preferred_element_type=f32)
            lat_buf[g, :, h + 1, :] = jnp.dot(odd, uk_buf[g, h + 1], preferred_element_type=f32)
        lat_out[0, g] = lat_buf[g].astype(bf16)
        pe_out[0, g] = pe_buf[g][:, :, :64].astype(bf16)
        for copy in swaps(g):
            copy.start()
        for copy in out_copies(0, g):
            copy.start()

        @pl.when(g >= 1)
        def _():
            receive(g - 1)
        return 0

    lax.fori_loop(0, n_groups, group, 0)

    receive(n_groups - 1)

    def drain(g, _):
        for half in range(2):
            for copy in out_copies(half, g):
                copy.wait()
        for copy in swaps(g):
            copy.wait_send()
        return 0

    lax.fori_loop(0, n_groups, drain, 0)
    cq_swap.wait_send()
    kv_swap.wait_send()


def project(hidden, cos_t, sin_t, w_dq, q_gain, w_uq, w_dkv_t, kv_gain, w_uk):
    n_seqs, d_model = hidden.shape
    q_lora = w_dq.shape[1]
    n_heads, nope, lat = w_uk.shape
    rope = w_uq.shape[1] // n_heads - nope
    tile = 8 * (nope + rope)
    n_groups = n_heads // 32
    n_dq, uq_slots = 4, 4
    f32, bf16 = jnp.float32, jnp.bfloat16
    hbm = pl.BlockSpec(memory_space=pl.ANY)
    vmem = pl.BlockSpec(memory_space=pltpu.VMEM)
    dma = pltpu.SemaphoreType.DMA
    return pl.pallas_call(
        functools.partial(project_kernel, n_seqs),
        out_shape=[
            jax.ShapeDtypeStruct((2, n_seqs, 64, lat), bf16),
            jax.ShapeDtypeStruct((2, n_seqs, 64, rope), bf16),
            jax.ShapeDtypeStruct((n_seqs, lat + rope), bf16),
            jax.ShapeDtypeStruct((n_seqs, lat), f32),
            jax.ShapeDtypeStruct((rope, 128), f32),
        ],
        in_specs=[vmem] * 5 + [hbm] * 4,
        out_specs=[hbm, hbm, vmem, vmem, vmem],
        scratch_shapes=[
            pltpu.VMEM((n_dq, d_model // (2 * n_dq), q_lora), bf16),
            pltpu.VMEM((lat + rope, d_model // 2), bf16),
            pltpu.VMEM((uq_slots, q_lora, tile), bf16),
            pltpu.VMEM((n_groups, 16, nope, lat), bf16),
            pltpu.VMEM((n_seqs, q_lora), f32),
            pltpu.VMEM((n_seqs, q_lora), f32),
            pltpu.VMEM((n_seqs, lat + rope), f32),
            pltpu.VMEM((n_seqs, lat + rope), f32),
            pltpu.VMEM((2, n_seqs, tile), f32),
            pltpu.VMEM((n_groups, n_seqs, 16, lat), f32),
            pltpu.VMEM((n_groups, n_seqs, 16, lat), f32),
            pltpu.VMEM((n_groups, n_seqs, 16, 128), f32),
            pltpu.VMEM((n_groups, n_seqs, 16, 128), f32),
            pltpu.VMEM((2, n_groups, n_seqs, 16, lat), bf16),
            pltpu.VMEM((2, n_groups, n_seqs, 16, rope), bf16),
            dma((n_dq,)), dma, dma((uq_slots,)), dma((n_groups,)), dma((2, n_groups)), dma((2, n_groups)), dma((2,)), dma((2,)),
            dma((n_groups,)), dma((n_groups,)), dma((n_groups,)), dma((n_groups,)),
        ],
        compiler_params=pltpu.CompilerParams(collective_id=1, has_side_effects=True, vmem_limit_bytes=60 * 1024 * 1024),
        name="project",
    )(hidden, q_gain, kv_gain, cos_t, sin_t, w_dq, w_dkv_t, w_uq, w_uk)


def attend_kernel(n_seqs, shard_len, scale, len_ref, cnew_ref, knew_ref, kv_ref, q_hbm, pe_hbm, ckv_hbm, kpe_hbm,
                  ckv_out, kpe_out, o_hbm, lse_ref, kv_out, cbuf, kbuf, qbuf, pbuf, obuf, s_scr, lse_scr, in_sem, out_sem, o_sem):
    step = pl.program_id(0)
    me = lax.axis_index("sp")
    chip = me // 2

    def copies_in(seq):
        slot = lax.rem(seq, NBUF)
        return (pltpu.make_async_copy(q_hbm.at[:, seq], qbuf.at[slot], in_sem.at[2, slot]),
                pltpu.make_async_copy(pe_hbm.at[:, seq], pbuf.at[slot], in_sem.at[3, slot]),
                pltpu.make_async_copy(kpe_hbm.at[seq], kbuf.at[slot], in_sem.at[1, slot]),
                pltpu.make_async_copy(ckv_hbm.at[seq], cbuf.at[slot], in_sem.at[0, slot]))

    def copies_out(seq):
        slot = lax.rem(seq, NBUF)
        return (pltpu.make_async_copy(cbuf.at[slot], ckv_out.at[seq], out_sem.at[0, slot]),
                pltpu.make_async_copy(kbuf.at[slot], kpe_out.at[seq], out_sem.at[1, slot]))

    def copy_o(seq):
        slot = lax.rem(seq, OBUF)
        return pltpu.make_async_copy(obuf.at[slot], o_hbm.at[:, :, seq], o_sem.at[slot])

    @pl.when(step == 0)
    def _():
        for seq in range(AHEAD):
            for copy in copies_in(jnp.int32(seq)):
                copy.start()

    ahead = step + AHEAD

    @pl.when(ahead < n_seqs)
    def _():
        @pl.when(ahead >= NBUF)
        def _():
            for copy in copies_out(ahead - NBUF):
                copy.wait()
        for copy in copies_in(ahead):
            copy.start()

    for copy in copies_in(step):
        copy.wait()
    slot = lax.rem(step, NBUF)
    pos = len_ref[step] - me * shard_len

    @pl.when((pos >= 0) & (pos < shard_len))
    def _():
        row0 = pl.multiple_of((pos // 16) * 16, 16)
        block = cbuf[slot, pl.ds(row0, 16), :].astype(jnp.float32)
        rows = lax.broadcasted_iota(jnp.int32, block.shape, 0) + row0
        cbuf[slot, pl.ds(row0, 16), :] = jnp.where(rows == pos, cnew_ref[pl.ds(step, 1), :], block).astype(jnp.bfloat16)
        col0 = pl.multiple_of((pos // 128) * 128, 128)
        seq_lane = lax.broadcasted_iota(jnp.int32, knew_ref.shape, 1) == step
        new_col = jnp.sum(jnp.where(seq_lane, knew_ref[...], 0.0), axis=1, keepdims=True)
        kblock = kbuf[slot, :, pl.ds(col0, 128)].astype(jnp.float32)
        cols = lax.broadcasted_iota(jnp.int32, kblock.shape, 1) + col0
        kbuf[slot, :, pl.ds(col0, 128)] = jnp.where(cols == pos, new_col, kblock).astype(jnp.bfloat16)

    q_lat = jnp.concatenate([qbuf[slot, 0], qbuf[slot, 1]], axis=0)
    q_pe = jnp.concatenate([pbuf[slot, 0], pbuf[slot, 1]], axis=0)
    peak = None
    for t0 in range(0, shard_len, TILE_T):
        s = lax.dot_general(q_lat, cbuf[slot, t0:t0 + TILE_T, :], (((1,), (1,)), ((), ())), preferred_element_type=jnp.float32)
        s = s + lax.dot_general(q_pe, kbuf[slot, :, t0:t0 + TILE_T], (((1,), (0,)), ((), ())), preferred_element_type=jnp.float32)
        cols = lax.broadcasted_iota(jnp.int32, s.shape, 1) + t0
        s = jnp.where(cols <= pos, s * scale, NEG_FILL)
        s_scr[:, t0:t0 + TILE_T] = s
        tile_peak = jnp.max(s, axis=1, keepdims=True)
        peak = tile_peak if peak is None else jnp.maximum(peak, tile_peak)
    denom = jnp.zeros_like(peak)
    acc = None
    for t0 in range(0, shard_len, TILE_T):
        w = jnp.exp(s_scr[:, t0:t0 + TILE_T] - peak)
        denom = denom + jnp.sum(w, axis=1, keepdims=True)
        part = jnp.dot(w.astype(jnp.bfloat16), cbuf[slot, t0:t0 + TILE_T, :], preferred_element_type=jnp.float32)
        acc = part if acc is None else acc + part
    for copy in copies_out(step):
        copy.start()
    o = acc * (1.0 / denom)
    oslot = lax.rem(step, OBUF)

    @pl.when(step >= OBUF)
    def _():
        copy_o(step - OBUF).wait()
    for half in range(2):
        for group in range(4):
            r0 = half * 64 + group * 16
            obuf[oslot, half, group ^ chip] = o[r0:r0 + 16, :]
    copy_o(step).start()
    lanes = lax.broadcasted_iota(jnp.int32, lse_scr.shape, 1)
    lse_scr[...] = jnp.where(lanes == step, peak + jnp.log(denom), lse_scr[...])

    @pl.when(step == n_seqs - 1)
    def _():
        lse_ref[...] = jnp.transpose(lse_scr[...])[:n_seqs, :]
        kv_out[...] = kv_ref[...]
        for seq in range(n_seqs - NBUF, n_seqs):
            for copy in copies_out(jnp.int32(seq)):
                copy.wait()
        for seq in range(n_seqs - OBUF, n_seqs):
            copy_o(jnp.int32(seq)).wait()


def attend(cache_len, q_lat, q_pe, c_new, k_new, kv_new, ckv, kpe_t, scale):
    n_seqs, shard_len, lat = ckv.shape
    rope = kpe_t.shape[1]
    whole = lambda shape: pl.BlockSpec(shape, lambda i, *_: (0,) * len(shape))
    hbm = pl.BlockSpec(memory_space=pl.ANY)
    return pl.pallas_call(
        functools.partial(attend_kernel, n_seqs, shard_len, scale),
        grid_spec=pltpu.PrefetchScalarGridSpec(
            num_scalar_prefetch=1,
            grid=(n_seqs,),
            in_specs=[whole((n_seqs, lat)), whole((rope, 128)), whole(kv_new.shape), hbm, hbm, hbm, hbm],
            out_specs=[hbm, hbm, hbm, whole((n_seqs, 128)), whole(kv_new.shape)],
            scratch_shapes=[
                pltpu.VMEM((NBUF, shard_len, lat), jnp.bfloat16),
                pltpu.VMEM((NBUF, rope, shard_len), jnp.bfloat16),
                pltpu.VMEM((NBUF, 2, 64, lat), jnp.bfloat16),
                pltpu.VMEM((NBUF, 2, 64, rope), jnp.bfloat16),
                pltpu.VMEM((OBUF, 2, 4, 16, lat), jnp.float32),
                pltpu.VMEM((128, shard_len), jnp.float32),
                pltpu.VMEM((128, 128), jnp.float32),
                pltpu.SemaphoreType.DMA((4, NBUF)),
                pltpu.SemaphoreType.DMA((2, NBUF)),
                pltpu.SemaphoreType.DMA((OBUF,)),
            ],
        ),
        out_shape=[
            jax.ShapeDtypeStruct(ckv.shape, ckv.dtype),
            jax.ShapeDtypeStruct(kpe_t.shape, kpe_t.dtype),
            jax.ShapeDtypeStruct((2, 4, n_seqs, 16, lat), jnp.float32),
            jax.ShapeDtypeStruct((n_seqs, 128), jnp.float32),
            jax.ShapeDtypeStruct(kv_new.shape, kv_new.dtype),
        ],
        compiler_params=pltpu.CompilerParams(dimension_semantics=("arbitrary",), vmem_limit_bytes=60 * 1024 * 1024),
        name="attend",
    )(cache_len, c_new, k_new, kv_new, q_lat, q_pe, ckv, kpe_t)


def combine_kernel(n_seqs, o_hbm, lse_ref, wuv_hbm, wout_hbm, out_ref, mine, got1, got2, got3, lse_all, w_mine, w_part,
                   wuv, wout, heads, part, part_got, quad, full, load_sem, wt_sem, d1_s, d1_r, s2_s, s2_r, s3_s, s3_r,
                   l_s, l_r, a_s, a_r, b_s, b_r, c_s, c_r, e_s, e_r):
    me = lax.axis_index("sp")
    core = lax.rem(me, 2)
    x_bit = lax.rem(me // 2, 2)
    y_bit = me // 4
    chip = me // 2

    def flip(bits):
        dev = me
        if bits & 1:
            dev = dev + 1 - 2 * core
        if bits & 2:
            dev = dev + 2 - 4 * x_bit
        if bits & 4:
            dev = dev + 4 - 8 * y_bit
        return dev

    def flip_chip(j):
        return (y_bit + (1 - 2 * y_bit if j & 2 else 0)) * 2 + x_bit + (1 - 2 * x_bit if j & 1 else 0)

    def send(src, dst, ssem, rsem, bits):
        return pltpu.make_async_remote_copy(src_ref=src, dst_ref=dst, send_sem=ssem, recv_sem=rsem,
                                            device_id={"sp": flip(bits)}, device_id_type=MESH)

    head0 = core * 64 + chip * 16
    wuv_copy = pltpu.make_async_copy(wuv_hbm.at[pl.ds(head0, 16)], wuv, wt_sem.at[0])
    wout_copy = pltpu.make_async_copy(wout_hbm.at[pl.ds(pl.multiple_of(head0 * 128, 2048), 2048)], wout, wt_sem.at[1])
    per_half = n_seqs // CHUNK
    n_chunks = 2 * per_half

    def span(c):
        return pl.ds((c % per_half) * CHUNK, CHUNK), pl.ds((c // per_half) * 8, 8)

    loads = []
    for c in range(n_chunks):
        seqs, hs = span(c)
        loads.append(pltpu.make_async_copy(o_hbm.at[0, :, seqs, hs], mine.at[:, seqs, hs], load_sem.at[c]))
        loads[c].start()

    barrier = pltpu.get_barrier_semaphore()
    for bits in range(1, 8):
        pl.semaphore_signal(barrier, inc=1, device_id={"sp": flip(bits)}, device_id_type=MESH)
    pl.semaphore_wait(barrier, 7)

    lse_sends = [send(lse_ref, lse_all.at[bits], l_s.at[bits], l_r.at[bits], bits) for bits in range(1, 8)]
    for copy in lse_sends:
        copy.start()
    d1 = []
    for c in range(n_chunks):
        seqs, hs = span(c)
        d1.append(send(o_hbm.at[1, :, seqs, hs], got1.at[:, seqs, hs], d1_s.at[c], d1_r.at[c], 1))
        d1[c].start()

    for copy in lse_sends:
        copy.wait_recv()
    lses = [lse_ref[...]]
    for bits in range(1, 8):
        other = lse_all[bits]
        lses.append(pltpu.roll(other, 64, 1) if bits & 1 else other)
    peak = functools.reduce(jnp.maximum, lses)
    total = functools.reduce(jnp.add, [jnp.exp(v - peak) for v in lses])
    norm = peak + jnp.log(total)
    pad = jnp.zeros((128 - n_seqs, 128), jnp.float32)
    for value, dst in ((lses[0], w_mine), (lses[1], w_part)):
        wt = jnp.transpose(jnp.concatenate([jnp.exp(value - norm), pad], axis=0))[:64, :]
        for s in range(n_seqs):
            dst[s] = jnp.broadcast_to(wt[:, s:s + 1], (64, 128))

    def orders(c):
        return (1, 2) if c % 2 == 0 else (2, 1)

    s2 = []
    for c in range(n_chunks):
        loads[c].wait()
        d1[c].wait_recv()
        seqs, hs = span(c)
        head = (c // per_half) * 8
        for j in range(4):
            row0 = pl.multiple_of(flip_chip(j) * 16 + head, 8)

            def merge(i, _, j=j, row0=row0, c=c, hs=hs):
                s = (c % per_half) * CHUNK + i
                wa = w_mine[s, pl.ds(row0, 8), :]
                wb = w_part[s, pl.ds(row0, 8), :]
                wa = jnp.concatenate([wa] * 4, axis=1)
                wb = jnp.concatenate([wb] * 4, axis=1)
                mine[j, s, hs] = mine[j, s, hs] * wa + got1[j, s, hs] * wb
                return 0

            lax.fori_loop(0, CHUNK, merge, 0, unroll=4)
        first, _ = orders(c)
        s2.append((send(mine.at[first, seqs, hs], got2.at[0, seqs, hs], s2_s.at[0, c], s2_r.at[0, c], 2 * first),
                   send(mine.at[3, seqs, hs], got2.at[1, seqs, hs], s2_s.at[1, c], s2_r.at[1, c], 2 * first)))
        for copy in s2[c]:
            copy.start()

    wuv_copy.start()
    wout_copy.start()

    s3 = []
    for c in range(n_chunks):
        _, second = orders(c)
        s2[c][0].wait_recv()
        s2[c][1].wait_recv()
        seqs, hs = span(c)
        mine[second, seqs, hs] = mine[second, seqs, hs] + got2[1, seqs, hs]
        s3.append(send(mine.at[second, seqs, hs], got3.at[seqs, hs], s3_s.at[c], s3_r.at[c], 2 * second))
        mine[0, seqs, hs] = mine[0, seqs, hs] + got2[0, seqs, hs]
        s3[c].start()

    def latents(c):
        s3[c].wait_recv()
        seqs, hs = span(c)
        mine[0, seqs, hs] = mine[0, seqs, hs] + got3[seqs, hs]

    def value_heads(h0):
        for h in range(h0, h0 + 8):
            x = mine[0, :, h, :].astype(jnp.bfloat16)
            o = lax.dot_general(x, wuv[h], (((1,), (1,)), ((), ())), preferred_element_type=jnp.float32)
            heads[:, h * 128:(h + 1) * 128] = o.astype(jnp.bfloat16)

    width = wout.shape[1] // 8
    depth = wout.shape[0] // 2

    for c in range(per_half):
        latents(c)
    wuv_copy.wait()
    value_heads(0)
    wout_copy.wait()
    for p in range(8):
        part[p // 4, p % 4] = jnp.dot(heads[:, :depth], wout[:depth, p * width:(p + 1) * width], preferred_element_type=jnp.float32)
    for c in range(per_half, n_chunks):
        latents(c)
    value_heads(8)

    def project_block(which, order):
        idx = flip_chip(order)
        col = pl.multiple_of((which * 4 + idx) * width, 128)
        part[which, idx] = part[which, idx] + jnp.dot(heads[:, depth:], wout[depth:, pl.ds(col, width)], preferred_element_type=jnp.float32)

    a = []
    for j in (3, 1, 2, 0):
        project_block(1 - core, j)
        idx = flip_chip(j)
        a.append(send(part.at[1 - core, idx], part_got.at[j], a_s.at[j], a_r.at[j], 1))
        a[-1].start()
    b = []
    for n, j in enumerate((3, 1, 2, 0)):
        project_block(core, j)
        idx = flip_chip(j)
        a[n].wait_recv()
        part[core, idx] = part[core, idx] + part_got[j]
        if j:
            b.append(send(part.at[core, idx], quad.at[j - 1], b_s.at[j - 1], b_r.at[j - 1], 2 * j))
            b[-1].start()
    for copy in b:
        copy.wait_recv()
    done = part[core, chip] + quad[0] + quad[1] + quad[2]
    full[core, chip] = done.astype(jnp.bfloat16).astype(jnp.float32)
    g = [send(full.at[core, chip], full.at[core, chip], c_s.at[j - 1], c_r.at[j - 1], 2 * j) for j in range(1, 4)]
    for copy in g:
        copy.start()
    e = []
    for n, j in enumerate((0, 2, 1, 3)):
        if j:
            g[j - 1].wait_recv()
        idx = flip_chip(j)
        e.append(send(full.at[core, idx], full.at[core, idx], e_s.at[j], e_r.at[j], 1))
        e[-1].start()
    for copy in e:
        copy.wait_recv()
    for p in range(8):
        out_ref[:, p * width:(p + 1) * width] = full[p // 4, p % 4].astype(jnp.bfloat16)

    for copy in lse_sends + d1 + [c for pair in s2 for c in pair] + s3 + a + b + g + e:
        copy.wait_send()


def combine(o_parts, lse, w_uv, w_out):
    _, _, n_seqs, _, lat = o_parts.shape
    d_model = w_out.shape[1]
    vdim = w_uv.shape[1]
    n_chunks = 2 * n_seqs // CHUNK
    width = d_model // 8
    hbm = pl.BlockSpec(memory_space=pl.ANY)
    vmem = pl.BlockSpec(memory_space=pltpu.VMEM)
    dma = pltpu.SemaphoreType.DMA
    f32 = jnp.float32
    return pl.pallas_call(
        functools.partial(combine_kernel, n_seqs),
        out_shape=jax.ShapeDtypeStruct((n_seqs, d_model), jnp.bfloat16),
        in_specs=[hbm, vmem, hbm, hbm],
        out_specs=vmem,
        scratch_shapes=[
            pltpu.VMEM((4, n_seqs, 16, lat), f32),
            pltpu.VMEM((4, n_seqs, 16, lat), f32),
            pltpu.VMEM((2, n_seqs, 16, lat), f32),
            pltpu.VMEM((n_seqs, 16, lat), f32),
            pltpu.VMEM((8, n_seqs, 128), f32),
            pltpu.VMEM((n_seqs, 64, 128), f32),
            pltpu.VMEM((n_seqs, 64, 128), f32),
            pltpu.VMEM((16, vdim, lat), jnp.bfloat16),
            pltpu.VMEM((16 * vdim, d_model), jnp.bfloat16),
            pltpu.VMEM((n_seqs, 16 * vdim), jnp.bfloat16),
            pltpu.VMEM((2, 4, n_seqs, width), f32),
            pltpu.VMEM((4, n_seqs, width), f32),
            pltpu.VMEM((3, n_seqs, width), f32),
            pltpu.VMEM((2, 4, n_seqs, width), f32),
            dma((n_chunks,)), dma((2,)),
            dma((n_chunks,)), dma((n_chunks,)),
            dma((2, n_chunks)), dma((2, n_chunks)),
            dma((n_chunks,)), dma((n_chunks,)),
            dma((8,)), dma((8,)),
            dma((4,)), dma((4,)), dma((3,)), dma((3,)), dma((3,)), dma((3,)), dma((4,)), dma((4,)),
        ],
        compiler_params=pltpu.CompilerParams(collective_id=0, has_side_effects=True, vmem_limit_bytes=60 * 1024 * 1024),
        name="combine",
    )(o_parts, lse, w_uv, w_out)


def solution(mesh):
    def local_step(hidden, ckv_blk, kpe_blk, cache_len, w_dq, q_gain, w_uq, w_dkv, kv_gain, w_uk, w_uv, w_out):
        rope = kpe_blk.shape[2]
        scale = (w_uk.shape[1] + rope) ** -0.5
        cos_t, sin_t = rope_tables(cache_len, rope)
        cos_t = jnp.concatenate([cos_t] * 4, axis=1)
        sin_t = jnp.concatenate([-sin_t, sin_t] * 2, axis=1)
        q_lat, q_pe, kv_new, c_new, k_new = project(hidden, cos_t, sin_t, w_dq, q_gain, w_uq, w_dkv.T, kv_gain, w_uk)
        ckv_out, kpe_out, o_parts, lse, kv_new = attend(cache_len, q_lat, q_pe, c_new, k_new, kv_new, ckv_blk, jnp.swapaxes(kpe_blk, 1, 2), scale)
        out = combine(o_parts, lse, w_uv, w_out)
        return out, ckv_out, jnp.swapaxes(kpe_out, 1, 2), kv_new

    cache_spec = P("dp", "sp", None)
    return jax.shard_map(local_step, mesh=mesh, in_specs=(P("dp", None), cache_spec, cache_spec, P("dp"), P(), P(), P(), P(), P(), P(), P(), P()), out_specs=(P("dp", None), cache_spec, cache_spec, P("dp", None)), check_vma=False)
```
